32 devices in a mesh: dp: 1 (over z), tp: 4 (over y), cp: 8 (over x, core).
Axes of the slice: x: 4, y: 4, z: 1, core: 2. Of those that a mesh axis runs over, the one named last changes fastest.
The devices are a block of a 4x4x8 slice.
Arguments:
- hidden: bfloat16 [2048, 5120], P(('dp', 'cp'))
- positions: int32 [2048], P(('dp', 'cp'))
- norm_gain: bfloat16 [5120], replicated
- w_query: bfloat16 [5120, 4096], P(None, 'tp')
- w_key: bfloat16 [5120, 1024], P(None, 'tp')
- w_value: bfloat16 [5120, 1024], P(None, 'tp')
- w_out: bfloat16 [4096, 5120], P('tp')
Outputs:
- output 1: bfloat16 [2048, 5120], P(('dp', 'cp'))
- output 2: bfloat16 [2048, 8, 128], P(('dp', 'cp'), 'tp')
- output 3: bfloat16 [2048, 8, 128], P(('dp', 'cp'), 'tp')
All inputs are finite; a program needn't handle non-finite values.
Results may differ from the reference program's by a relative error of at most 0.00862386.
Values are sent between devices in bfloat16 or wider.
A program may use at most 768 MiB of HBM per device.

```python
import math
import jax
import jax.numpy as jnp
from jax import lax

D = 5120
HEADS = 32
KV_HEADS = 8
HEAD = 128
SEQ = 2048
Q_ROWS = 128

EPS = 1e-5
LOG_THETA = math.log(1000000.0)


def setup_inputs(seed: int = 0, part: int = 0) -> dict:
    base_key = jax.random.key(seed)
    shared = jax.random.split(base_key, 5)
    part_keys = jax.random.split(jax.random.fold_in(base_key, part), 3)
    sharpness = math.sqrt(math.log(SEQ / 16.0))
    hidden = 0.5 * jax.random.normal(part_keys[0], (SEQ, D), jnp.float32)
    first_pos = jax.random.randint(part_keys[1], (), 0, SEQ, dtype=jnp.int32)
    pos_steps = jax.random.randint(part_keys[2], (SEQ,), 1, 3, dtype=jnp.int32)
    positions = (first_pos + jnp.cumsum(pos_steps) - 1).astype(jnp.int32)
    norm_gain = 1.0 + 0.3 * jax.random.normal(shared[0], (D,), jnp.float32)
    w_query = (sharpness / math.sqrt(D)) * jax.random.normal(shared[1], (D, HEADS * HEAD), jnp.float32)
    w_key = jax.random.normal(shared[2], (D, KV_HEADS * HEAD), jnp.float32) / math.sqrt(D)
    w_value = jax.random.normal(shared[3], (D, KV_HEADS * HEAD), jnp.float32) / math.sqrt(D)
    w_out = jax.random.normal(shared[4], (HEADS * HEAD, D), jnp.float32) / math.sqrt(HEADS * HEAD)
    return {
        'hidden': hidden.astype(jnp.bfloat16),
        'positions': positions,
        'norm_gain': norm_gain.astype(jnp.bfloat16),
        'w_query': w_query.astype(jnp.bfloat16),
        'w_key': w_key.astype(jnp.bfloat16),
        'w_value': w_value.astype(jnp.bfloat16),
        'w_out': w_out.astype(jnp.bfloat16),
    }


def rope_tables(positions):
    half_dim = HEAD // 2
    inv_freq = jnp.exp(jnp.arange(half_dim, dtype=jnp.float32) * (-2.0 * LOG_THETA / HEAD))
    angles = positions.astype(jnp.float32)[..., None] * inv_freq
    return jnp.cos(angles), jnp.sin(angles)


def apply_rope(head_vals, cos_t, sin_t):
    half_dim = HEAD // 2
    first_half = head_vals[..., :half_dim]
    second_half = head_vals[..., half_dim:]
    return jnp.concatenate([first_half * cos_t - second_half * sin_t, second_half * cos_t + first_half * sin_t], axis=-1)


def reference(hidden, positions, norm_gain, w_query, w_key, w_value, w_out):
    group_size = HEADS // KV_HEADS
    tile_count = SEQ // Q_ROWS
    hidden_f = hidden.astype(jnp.float32)
    inv_rms = lax.rsqrt(jnp.mean(hidden_f * hidden_f, axis=-1, keepdims=True) + EPS)
    normed = (hidden_f * inv_rms * norm_gain.astype(jnp.float32)).astype(jnp.bfloat16)
    cos_t, sin_t = rope_tables(positions)
    cos_b = cos_t[:, None, :]
    sin_b = sin_t[:, None, :]
    q_proj = jnp.dot(normed, w_query, preferred_element_type=jnp.float32).reshape(SEQ, HEADS, HEAD)
    k_proj = jnp.dot(normed, w_key, preferred_element_type=jnp.float32).reshape(SEQ, KV_HEADS, HEAD)
    queries = apply_rope(q_proj, cos_b, sin_b).astype(jnp.bfloat16)
    k_rope = apply_rope(k_proj, cos_b, sin_b).astype(jnp.bfloat16)
    values = jnp.dot(normed, w_value, preferred_element_type=jnp.float32).astype(jnp.bfloat16).reshape(SEQ, KV_HEADS, HEAD)
    q_tiles = queries.astype(jnp.float32).reshape(tile_count, Q_ROWS, KV_HEADS, group_size, HEAD)
    pos_tiles = positions.reshape(tile_count, Q_ROWS)
    k_full = k_rope.astype(jnp.float32)
    v_full = values.astype(jnp.float32)
    score_scale = 1.0 / math.sqrt(HEAD)

    def one_tile(tile_in):
        q_tile, q_pos = tile_in
        scores = jnp.einsum('qngd,knd->ngqk', q_tile, k_full) * score_scale
        visible = positions[None, :] <= q_pos[:, None]
        scores = jnp.where(visible, scores, -jnp.inf)
        weights = jax.nn.softmax(scores, axis=-1)
        return jnp.einsum('ngqk,knd->qngd', weights, v_full)

    attn_tiles = lax.map(one_tile, (q_tiles, pos_tiles))
    attn_o = attn_tiles.reshape(SEQ, HEADS * HEAD).astype(jnp.bfloat16)
    attn_sum = jnp.dot(attn_o, w_out, preferred_element_type=jnp.float32)
    hidden_out = (hidden_f + attn_sum).astype(jnp.bfloat16)
    return hidden_out, k_rope, values
```

```python
import math
import functools
import jax
import jax.numpy as jnp
from jax import lax
from jax.experimental import pallas as pl
from jax.experimental.pallas import tpu as pltpu
from jax.sharding import PartitionSpec as P

HEAD = 128
EPS = 1e-5
LOG_THETA = math.log(1000000.0)
EXP2_SCALE = math.log2(math.e) / math.sqrt(HEAD)
MESH = pl.DeviceIdType.MESH
F32 = jnp.float32
BF16 = jnp.bfloat16
DISTANCES = (1, 3, 2)


def block_kernel(tp_n, cp_n, x_hbm, pos_ref, freq_ref, gain_ref, wq_hbm, wk_hbm, wv_hbm, wo_hbm,
                 out_hbm, k_hbm, v_hbm,
                 x_v, h_v, wkv_v, wq_v, wo_v, cos_v, sin_v, q_v, kv_v, kvo_v, m_v, l_v, acc_v, o_v,
                 part_v, sbuf, rbuf, out_v,
                 x_sem, wkv_sem, wq_sem, wo_sem, cache_sem, out_sem,
                 kv_send, kv_recv, fwd_send, fwd_recv, sib_send, sib_recv,
                 rs_send, rs_recv, ag_send, ag_recv):
    rows, width = x_v.shape
    chips = cp_n // 2
    heads = q_v.shape[0]
    kv_heads = kv_v.shape[0] // 2
    group = heads // kv_heads
    half = rows // 2
    chunk = width // tp_n
    sub = chunk // 2
    ty = lax.axis_index('tp')
    c_me = lax.axis_index('cp')
    chip = c_me // 2
    core = lax.rem(c_me, 2)
    sibling = chip * 2 + (1 - core)

    x_copy = pltpu.make_async_copy(x_hbm, x_v, x_sem)
    x_copy.start()
    kvw = kv_heads * HEAD
    wkv_copies = [pltpu.make_async_copy(wk_hbm, wkv_v.at[:, pl.ds(0, kvw)], wkv_sem.at[0]),
                  pltpu.make_async_copy(wv_hbm, wkv_v.at[:, pl.ds(kvw, kvw)], wkv_sem.at[1])]
    for cp in wkv_copies:
        cp.start()
    qw = wq_v.shape[1] // 2
    wq_copies = [pltpu.make_async_copy(wq_hbm.at[:, pl.ds(j * qw, qw)], wq_v.at[:, pl.ds(j * qw, qw)], wq_sem.at[j]) for j in range(2)]
    for cp in wq_copies:
        cp.start()
    wo_copy = pltpu.make_async_copy(wo_hbm, wo_v, wo_sem)
    wo_copy.start()

    barrier = pltpu.get_barrier_semaphore()
    y_next = lax.rem(ty + 1, tp_n)
    y_prev = lax.rem(ty + tp_n - 1, tp_n)
    partners = [{'tp': y_next}, {'tp': y_prev}, {'cp': sibling}]
    for d in range(1, chips):
        partners.append({'cp': lax.rem(c_me + 2 * d, cp_n)})
    for dev in partners:
        pl.semaphore_signal(barrier, inc=1, device_id=dev, device_id_type=MESH)

    angles = freq_ref[...] * pos_ref[...].astype(F32)
    cos_t = jnp.cos(angles)
    sin_t = jnp.sin(angles)
    cos_v[...] = jnp.concatenate([cos_t, cos_t], axis=0).T
    sin_v[...] = jnp.concatenate([-sin_t, sin_t], axis=0).T

    x_copy.wait()
    strip = 32

    def norm_strip(i, carry):
        r = pl.ds(pl.multiple_of(i * strip, strip), strip)
        xf = x_v[r, :].astype(F32)
        inv = lax.rsqrt(jnp.mean(xf * xf, axis=-1, keepdims=True) + EPS)
        h_v[r, :] = (xf * inv * gain_ref[...].astype(F32)).astype(BF16)
        return carry
    lax.fori_loop(0, rows // strip, norm_strip, 0)

    def rope(t):
        return t * cos_v[...] + pltpu.roll(t, HEAD // 2, 1) * sin_v[...]

    for cp in wkv_copies:
        cp.wait()
    kv_f = jnp.dot(h_v[...], wkv_v[...], preferred_element_type=F32)
    own_rows = pl.ds(pl.multiple_of(c_me * rows, rows), rows)
    for i in range(kv_heads):
        k_h = rope(kv_f[:, i * HEAD:(i + 1) * HEAD]).astype(BF16)
        kv_v[i, own_rows, :] = k_h
        kvo_v[0, :, i * HEAD:(i + 1) * HEAD] = k_h
        v_h = kv_f[:, kvw + i * HEAD:kvw + (i + 1) * HEAD].astype(BF16)
        kv_v[kv_heads + i, own_rows, :] = v_h
        kvo_v[1, :, i * HEAD:(i + 1) * HEAD] = v_h

    pl.semaphore_wait(barrier, len(partners))

    def kv_rows(c):
        return pl.ds(pl.multiple_of(c * rows, rows), rows)

    def kv_copy(src_c, target_c, ssem, rsem):
        ref = kv_v.at[:, kv_rows(src_c), :]
        return pltpu.make_async_remote_copy(src_ref=ref, dst_ref=ref, send_sem=ssem, recv_sem=rsem,
                                            device_id={'cp': target_c}, device_id_type=MESH)

    @pl.when(core == 0)
    def _():
        kv_copy(c_me, sibling, sib_send, sib_recv).start()
    for d in DISTANCES:
        @pl.when(chip + d < chips)
        def _(d=d):
            kv_copy(c_me, lax.rem(c_me + 2 * d, cp_n), kv_send.at[d - 1], kv_recv.at[d - 1]).start()
    k_cache = pltpu.make_async_copy(kvo_v.at[0], k_hbm, cache_sem.at[0])
    v_cache = pltpu.make_async_copy(kvo_v.at[1], v_hbm, cache_sem.at[1])
    k_cache.start()
    v_cache.start()

    for j in range(2):
        wq_copies[j].wait()
        q_f = jnp.dot(h_v[...], wq_v[:, j * qw:(j + 1) * qw], preferred_element_type=F32)
        for i in range(qw // HEAD):
            q_v[j * (qw // HEAD) + i] = rope(q_f[:, i * HEAD:(i + 1) * HEAD]).astype(BF16)

    def fold(p):
        out = p[:, 0:HEAD]
        for i in range(1, p.shape[1] // HEAD):
            out = out + p[:, i * HEAD:(i + 1) * HEAD]
        return out

    def own_head(hd, carry):
        kh = hd // group
        s = lax.dot_general(q_v[hd], kv_v[kh, own_rows, :], (((1,), (1,)), ((), ())), preferred_element_type=F32)
        r_i = lax.broadcasted_iota(jnp.int32, s.shape, 0)
        c_i = lax.broadcasted_iota(jnp.int32, s.shape, 1)
        s = jnp.where(c_i <= r_i, s, -jnp.inf)
        m = jnp.max(s, axis=1, keepdims=True)
        p = jnp.exp2((s - m) * EXP2_SCALE)
        m_v[hd] = jnp.broadcast_to(m, (rows, HEAD))
        l_v[hd] = fold(p)
        acc_v[hd] = jnp.dot(p.astype(BF16), kv_v[kv_heads + kh, own_rows, :], preferred_element_type=F32)
        return carry
    lax.fori_loop(0, heads, own_head, 0)

    def attend(start, count):
        keys = pl.ds(pl.multiple_of(start, rows), count)

        def one_head(hd, carry):
            kh = hd // group
            s = lax.dot_general(q_v[hd], kv_v[kh, keys, :], (((1,), (1,)), ((), ())), preferred_element_type=F32)
            m_old = m_v[hd]
            m_new = jnp.maximum(m_old, jnp.max(s, axis=1, keepdims=True))
            alpha = jnp.exp2((m_old - m_new) * EXP2_SCALE)
            p = jnp.exp2((s - m_new[:, 0:1]) * EXP2_SCALE)
            m_v[hd] = m_new
            l_v[hd] = l_v[hd] * alpha + fold(p)
            acc_v[hd] = acc_v[hd] * alpha + jnp.dot(p.astype(BF16), kv_v[kv_heads + kh, keys, :], preferred_element_type=F32)
            return carry
        lax.fori_loop(0, heads, one_head, 0)

    @pl.when(core == 1)
    def _():
        kv_copy(sibling, c_me, sib_send, sib_recv).wait_recv()
        attend(sibling * rows, rows)

    for d in DISTANCES:
        @pl.when(chip >= d)
        def _(d=d):
            src = c_me - 2 * d
            kv_copy(src, c_me, kv_send.at[d - 1], kv_recv.at[d - 1]).wait_recv()
            fwd = kv_copy(src, sibling, fwd_send.at[d - 1], fwd_recv.at[d - 1])
            fwd.start()
            other = sibling - 2 * d
            kv_copy(other, c_me, fwd_send.at[d - 1], fwd_recv.at[d - 1]).wait_recv()
            attend((chip - d) * 2 * rows, 2 * rows)

    def finish_head(hd, carry):
        total = jnp.sum(l_v[hd], axis=1, keepdims=True)
        o_v[:, pl.ds(pl.multiple_of(hd * HEAD, HEAD), HEAD)] = (acc_v[hd] / total).astype(BF16)
        return carry
    lax.fori_loop(0, heads, finish_head, 0)

    wo_copy.wait()
    targets = (y_next, y_prev)
    dir_rows = (pl.ds(0, half), pl.ds(half, half))
    subs = (pl.ds(0, sub), pl.ds(sub, sub))

    def rs_copy(dr, s, u):
        return pltpu.make_async_remote_copy(
            src_ref=sbuf.at[dr, s, :, subs[u]], dst_ref=rbuf.at[dr, s, :, subs[u]],
            send_sem=rs_send.at[dr, s, u], recv_sem=rs_recv.at[dr, s, u],
            device_id={'tp': targets[dr]}, device_id_type=MESH)

    def ag_copy(dr, a, u, idx):
        ref = out_v.at[idx, dir_rows[dr], subs[u]]
        return pltpu.make_async_remote_copy(
            src_ref=ref, dst_ref=ref, send_sem=ag_send.at[dr, a, u], recv_sem=ag_recv.at[dr, a, u],
            device_id={'tp': targets[dr]}, device_id_type=MESH)

    order = (y_prev, y_next, lax.rem(ty + 2, tp_n), ty)
    for i in range(tp_n):
        cols = pl.ds(pl.multiple_of(order[i] * chunk, HEAD), chunk)
        part = jnp.dot(o_v[...], wo_v[:, cols], preferred_element_type=F32)
        part_v[i] = part
        if i < 2:
            sbuf[i, 0] = part[i * half:(i + 1) * half].astype(BF16)
            for u in range(2):
                rs_copy(i, 0, u).start()

    use = ((2, 1), (2, 0))
    for s in (1, 2):
        for u in range(2):
            for dr in range(2):
                rs_copy(dr, s - 1, u).wait_recv()
                got = rbuf[dr, s - 1, :, subs[u]].astype(F32)
                sbuf[dr, s, :, subs[u]] = (got + part_v[use[dr][s - 1], dir_rows[dr], subs[u]]).astype(BF16)
                rs_copy(dr, s, u).start()

    def out_copy(dr, a, u, idx):
        cols = pl.ds(pl.multiple_of(idx * chunk + u * sub, HEAD), sub)
        return pltpu.make_async_copy(out_v.at[idx, dir_rows[dr], subs[u]], out_hbm.at[dir_rows[dr], cols], out_sem.at[dr, a, u])

    for u in range(2):
        for dr in range(2):
            rs_copy(dr, 2, u).wait_recv()
            cols = pl.ds(pl.multiple_of(ty * chunk + u * sub, HEAD), sub)
            a_sum = rbuf[dr, 2, :, subs[u]].astype(F32) + part_v[3, dir_rows[dr], subs[u]]
            out_v[ty, dir_rows[dr], subs[u]] = (x_v[dir_rows[dr], cols].astype(F32) + a_sum).astype(BF16)
            ag_copy(dr, 0, u, ty).start()
            out_copy(dr, 0, u, ty).start()

    def held(dr, a):
        return lax.rem(ty + tp_n - a, tp_n) if dr == 0 else lax.rem(ty + a, tp_n)

    for a in range(1, tp_n):
        for u in range(2):
            for dr in range(2):
                idx = held(dr, a)
                ag_copy(dr, a - 1, u, idx).wait_recv()
                if a < tp_n - 1:
                    ag_copy(dr, a, u, idx).start()
                out_copy(dr, a, u, idx).start()

    for a in range(tp_n):
        for u in range(2):
            for dr in range(2):
                out_copy(dr, a, u, held(dr, a)).wait()
                if a < tp_n - 1:
                    rs_copy(dr, a, u).wait_send()
                    ag_copy(dr, a, u, held(dr, a)).wait_send()
    k_cache.wait()
    v_cache.wait()

    @pl.when(core == 0)
    def _():
        kv_copy(c_me, sibling, sib_send, sib_recv).wait_send()
    for d in DISTANCES:
        @pl.when(chip + d < chips)
        def _(d=d):
            kv_copy(c_me, lax.rem(c_me + 2 * d, cp_n), kv_send.at[d - 1], kv_recv.at[d - 1]).wait_send()

        @pl.when(chip >= d)
        def _(d=d):
            kv_copy(c_me - 2 * d, sibling, fwd_send.at[d - 1], fwd_recv.at[d - 1]).wait_send()


def solution(mesh):
    tp_n = mesh.shape['tp']
    cp_n = mesh.shape['cp']
    row_spec = P(('dp', 'cp'), None)
    cache_spec = P(('dp', 'cp'), 'tp', None)
    head_cols = P(None, 'tp')

    def local_block(hidden, positions, norm_gain, w_query, w_key, w_value, w_out):
        rows, width = hidden.shape
        q_cols = w_query.shape[1]
        kv_cols = w_key.shape[1]
        heads = q_cols // HEAD
        kv_heads = kv_cols // HEAD
        chunk = width // tp_n
        half = rows // 2
        inv_freq = jnp.exp(jnp.arange(HEAD // 2, dtype=F32) * (-2.0 * LOG_THETA / HEAD))
        any_spec = pl.BlockSpec(memory_space=pl.ANY)
        vmem_spec = pl.BlockSpec(memory_space=pltpu.VMEM)
        dma = pltpu.SemaphoreType.DMA
        out, k_flat, v_flat = pl.pallas_call(
            functools.partial(block_kernel, tp_n, cp_n),
            out_shape=(jax.ShapeDtypeStruct((rows, width), BF16),
                       jax.ShapeDtypeStruct((rows, kv_cols), BF16),
                       jax.ShapeDtypeStruct((rows, kv_cols), BF16)),
            in_specs=[any_spec, vmem_spec, vmem_spec, vmem_spec, any_spec, any_spec, any_spec, any_spec],
            out_specs=(any_spec, any_spec, any_spec),
            scratch_shapes=[
                pltpu.VMEM((rows, width), BF16),
                pltpu.VMEM((rows, width), BF16),
                pltpu.VMEM((width, 2 * kv_cols), BF16),
                pltpu.VMEM((width, q_cols), BF16),
                pltpu.VMEM((q_cols, width), BF16),
                pltpu.VMEM((rows, HEAD), F32),
                pltpu.VMEM((rows, HEAD), F32),
                pltpu.VMEM((heads, rows, HEAD), BF16),
                pltpu.VMEM((2 * kv_heads, cp_n * rows, HEAD), BF16),
                pltpu.VMEM((2, rows, kv_cols), BF16),
                pltpu.VMEM((heads, rows, HEAD), F32),
                pltpu.VMEM((heads, rows, HEAD), F32),
                pltpu.VMEM((heads, rows, HEAD), F32),
                pltpu.VMEM((rows, q_cols), BF16),
                pltpu.VMEM((tp_n, rows, chunk), F32),
                pltpu.VMEM((2, tp_n - 1, half, chunk), BF16),
                pltpu.VMEM((2, tp_n - 1, half, chunk), BF16),
                pltpu.VMEM((tp_n, rows, chunk), BF16),
                dma, dma((2,)), dma((2,)), dma, dma((2,)), dma((2, tp_n, 2)),
                dma((3,)), dma((3,)), dma((3,)), dma((3,)), dma, dma,
                dma((2, tp_n - 1, 2)), dma((2, tp_n - 1, 2)), dma((2, tp_n - 1, 2)), dma((2, tp_n - 1, 2)),
            ],
            compiler_params=pltpu.CompilerParams(collective_id=0, has_side_effects=True, vmem_limit_bytes=64 * 1024 * 1024 - 65536),
        )(hidden, positions.reshape(1, rows), inv_freq.reshape(HEAD // 2, 1), norm_gain.reshape(1, width), w_query, w_key, w_value, w_out)
        return out, k_flat.reshape(rows, kv_heads, HEAD), v_flat.reshape(rows, kv_heads, HEAD)

    return jax.shard_map(local_block, mesh=mesh, in_specs=(row_spec, P(('dp', 'cp')), P(None), head_cols, head_cols, head_cols, P('tp', None)), out_specs=(row_spec, cache_spec, cache_spec), check_vma=False)
```

```python
import math
import functools
import jax
import jax.numpy as jnp
from jax import lax
from jax.experimental import pallas as pl
from jax.experimental.pallas import tpu as pltpu
from jax.sharding import PartitionSpec as P

HEAD = 128
EPS = 1e-5
LOG_THETA = math.log(1000000.0)
EXP2_SCALE = math.log2(math.e) / math.sqrt(HEAD)
MESH = pl.DeviceIdType.MESH
F32 = jnp.float32
BF16 = jnp.bfloat16
UNROLL = 4
VMEM_LIMIT = 56 * 1024 * 1024


def block_kernel(tp_n, cp_n, x_hbm, pos_ref, gain_ref, wq_hbm, wk_hbm, wv_hbm, wo_hbm,
                 out_v, k_out, v_out,
                 x_v, h_v, wkv_v, wq_v, wo_v, gain_v, cos_v, sin_v, q_v, kv_v, m_v, l_v, acc_v, o_v,
                 part_v, sbuf, rbuf,
                 x_sem, wkv_sem, wq_sem, wo_sem,
                 own_send, relay_send, fwd_send, kv_recv, fwd_recv,
                 rs_send, rs_recv, ag_send, ag_recv):
    rows, width = x_v.shape
    chips = cp_n // 2
    heads = q_v.shape[0]
    kv_heads = kv_v.shape[0]
    group = heads // kv_heads
    half = rows // 2
    chunk = width // tp_n
    sub = chunk // 2
    ty = lax.axis_index('tp')
    c_me = lax.axis_index('cp')
    chip = c_me // 2
    core = lax.rem(c_me, 2)
    sibling = chip * 2 + (1 - core)

    x_copy = pltpu.make_async_copy(x_hbm, x_v, x_sem)
    x_copy.start()
    kvw = kv_heads * HEAD
    wkv_copies = [pltpu.make_async_copy(wk_hbm, wkv_v.at[:, pl.ds(0, kvw)], wkv_sem.at[0]),
                  pltpu.make_async_copy(wv_hbm, wkv_v.at[:, pl.ds(kvw, kvw)], wkv_sem.at[1])]
    for cp in wkv_copies:
        cp.start()
    qw = wq_v.shape[1] // 2
    wq_copies = [pltpu.make_async_copy(wq_hbm.at[:, pl.ds(j * qw, qw)], wq_v.at[:, pl.ds(j * qw, qw)], wq_sem.at[j]) for j in range(2)]
    wo_copy = pltpu.make_async_copy(wo_hbm, wo_v, wo_sem)

    barrier = pltpu.get_barrier_semaphore()
    y_next = lax.rem(ty + 1, tp_n)
    y_prev = lax.rem(ty + tp_n - 1, tp_n)
    partners = [{'tp': y_next}, {'tp': y_prev}, {'cp': sibling}]
    for d in range(1, chips):
        partners.append({'cp': lax.rem(c_me + 2 * d, cp_n)})
    for dev in partners:
        pl.semaphore_signal(barrier, inc=1, device_id=dev, device_id_type=MESH)

    freq = jnp.exp(lax.broadcasted_iota(jnp.int32, (HEAD // 2, rows), 0).astype(F32) * (-2.0 * LOG_THETA / HEAD))
    angles = pos_ref[...].astype(F32) * freq
    cos_t = jnp.cos(angles)
    sin_t = jnp.sin(angles)
    cos_v[...] = jnp.concatenate([cos_t, cos_t], axis=0).T
    sin_v[...] = jnp.concatenate([-sin_t, sin_t], axis=0).T

    gain_f = gain_ref[...].astype(F32)
    for i in range(width // HEAD):
        gain_v[:, i * HEAD:(i + 1) * HEAD] = gain_f[i:i + 1, :]

    x_copy.wait()
    for cp in wq_copies:
        cp.start()
    strip = 32

    def norm_strip(i, carry):
        r = pl.ds(pl.multiple_of(i * strip, strip), strip)
        xf = x_v[r, :].astype(F32)
        inv = lax.rsqrt(jnp.mean(xf * xf, axis=-1, keepdims=True) + EPS)
        h_v[r, :] = (xf * inv * gain_v[...]).astype(BF16)
        return carry
    lax.fori_loop(0, rows // strip, norm_strip, 0)

    def rope(t):
        return t * cos_v[...] + pltpu.roll(t, HEAD // 2, 1) * sin_v[...]

    for cp in wkv_copies:
        cp.wait()
    kv_f = jnp.dot(h_v[...], wkv_v[...], preferred_element_type=F32)
    wo_copy.start()

    def kv_rows(c):
        return pl.ds(pl.multiple_of(c * rows, rows), rows)

    own_rows = kv_rows(c_me)
    for i in range(kv_heads):
        k_h = rope(kv_f[:, i * HEAD:(i + 1) * HEAD]).astype(BF16)
        kv_v[i, 0, own_rows, :] = k_h
        v_h = kv_f[:, kvw + i * HEAD:kvw + (i + 1) * HEAD].astype(BF16)
        kv_v[i, 1, own_rows, :] = v_h

    pl.semaphore_wait(barrier, len(partners))

    def kv_copy(h, src_c, target_c, ssem, rsem):
        ref = kv_v.at[h, :, kv_rows(src_c), :]
        return pltpu.make_async_remote_copy(src_ref=ref, dst_ref=ref, send_sem=ssem, recv_sem=rsem,
                                            device_id={'cp': target_c}, device_id_type=MESH)

    def at_chip(i):
        return i * 2 + core

    plan = ((0, 3, (0, 1), 0), (0, 1, (0, 1), 1), (1, 0, (1,), 0), (1, 2, (0, 1), 1), (2, 3, (0, 1), 1))

    def own_copy(to, h, slot):
        return kv_copy(h, c_me, at_chip(to), own_send.at[slot, h], kv_recv.at[chip, h])

    def sib_copy(h):
        return kv_copy(h, c_me, sibling, fwd_send.at[chip, h], fwd_recv.at[chip, h])

    for frm in range(chips):
        @pl.when(chip == frm)
        def _(frm=frm):
            for h in range(kv_heads):
                for a, to, hs, slot in plan:
                    if a == frm and h in hs:
                        own_copy(to, h, slot).start()

    @pl.when(core == 0)
    def _():
        for h in range(kv_heads):
            sib_copy(h).start()

    for j in range(2):
        wq_copies[j].wait()
        q_f = jnp.dot(h_v[...], wq_v[:, j * qw:(j + 1) * qw], preferred_element_type=F32)
        for i in range(qw // HEAD):
            q_v[j * (qw // HEAD) + i] = rope(q_f[:, i * HEAD:(i + 1) * HEAD]).astype(BF16)

    def fold(p):
        out = p[:, 0:HEAD]
        for i in range(1, p.shape[1] // HEAD):
            out = out + p[:, i * HEAD:(i + 1) * HEAD]
        return out

    def scores(hd, kh, keys):
        return lax.dot_general(q_v[hd], kv_v[kh, 0, keys, :], (((1,), (1,)), ((), ())), preferred_element_type=F32)

    def own_heads(i, carry):
        hds = [i * UNROLL + u for u in range(UNROLL)]
        kh = hds[0] // group
        ss = [scores(hd, kh, own_rows) for hd in hds]
        r_i = lax.broadcasted_iota(jnp.int32, (rows, rows), 0)
        c_i = lax.broadcasted_iota(jnp.int32, (rows, rows), 1)
        ss = [jnp.where(c_i <= r_i, s, -jnp.inf) for s in ss]
        ms = [jnp.max(s, axis=1, keepdims=True) for s in ss]
        ps = [jnp.exp2((s - m) * EXP2_SCALE) for s, m in zip(ss, ms)]
        vals = kv_v[kh, 1, own_rows, :]
        accs = [jnp.dot(p.astype(BF16), vals, preferred_element_type=F32) for p in ps]
        for hd, m, p, acc in zip(hds, ms, ps, accs):
            m_v[hd] = jnp.broadcast_to(m, (rows, HEAD))
            l_v[hd] = fold(p)
            acc_v[hd] = acc
        return carry
    lax.fori_loop(0, heads // UNROLL, own_heads, 0)

    def attend(start, count):
        keys = pl.ds(pl.multiple_of(start, rows), count)

        def some_heads(i, carry):
            hds = [i * UNROLL + u for u in range(UNROLL)]
            kh = hds[0] // group
            ss = [scores(hd, kh, keys) for hd in hds]
            olds = [m_v[hd] for hd in hds]
            ls = [l_v[hd] for hd in hds]
            accs = [acc_v[hd] for hd in hds]
            news = [jnp.maximum(m, jnp.max(s, axis=1, keepdims=True)) for m, s in zip(olds, ss)]
            alphas = [jnp.exp2((m - n) * EXP2_SCALE) for m, n in zip(olds, news)]
            ps = [jnp.exp2((s - n[:, 0:1]) * EXP2_SCALE) for s, n in zip(ss, news)]
            vals = kv_v[kh, 1, keys, :]
            pvs = [jnp.dot(p.astype(BF16), vals, preferred_element_type=F32) for p in ps]
            for hd, n, l, a, p, acc, pv in zip(hds, news, ls, alphas, ps, accs, pvs):
                m_v[hd] = n
                l_v[hd] = l * a + fold(p)
                acc_v[hd] = acc * a + pv
            return carry
        lax.fori_loop(0, heads // UNROLL, some_heads, 0)

    def sib_wait(i, h):
        kv_copy(h, 2 * i + 1 - core, c_me, fwd_send.at[i, h], fwd_recv.at[i, h]).wait_recv()

    @pl.when(chip == 0)
    def _():
        kv_copy(1, at_chip(1), c_me, relay_send.at[0], kv_recv.at[1, 1]).wait_recv()
        kv_copy(1, at_chip(1), at_chip(3), relay_send.at[0], kv_recv.at[1, 1]).start()

    @pl.when(core == 1)
    def _():
        for h in range(kv_heads):
            sib_wait(chip, h)
        attend(sibling * rows, rows)

    for t in range(chips - 1):
        @pl.when(t < chip)
        def _(t=t):
            src = lax.rem(chip - 1 + chip // 3 - t + 3, 3)
            for h in range(kv_heads):
                kv_copy(h, at_chip(src), c_me, own_send.at[0, h], kv_recv.at[src, h]).wait_recv()
                if t == 0:
                    @pl.when(chip == 3)
                    def _():
                        kv_copy(h, at_chip(0), at_chip(2), relay_send.at[h], kv_recv.at[0, h]).start()
                    if h == 0:
                        @pl.when(chip == 2)
                        def _():
                            kv_copy(h, at_chip(1), at_chip(3), relay_send.at[0], kv_recv.at[1, h]).start()
                kv_copy(h, at_chip(src), sibling, fwd_send.at[src, h], fwd_recv.at[src, h]).start()
            for h in range(kv_heads):
                sib_wait(src, h)
            attend(src * 2 * rows, 2 * rows)

    def finish_head(hd, carry):
        total = jnp.sum(l_v[hd], axis=1, keepdims=True)
        o_v[:, pl.ds(pl.multiple_of(hd * HEAD, HEAD), HEAD)] = (acc_v[hd] / total).astype(BF16)
        return carry
    lax.fori_loop(0, heads, finish_head, 0)

    wo_copy.wait()
    targets = (y_next, y_prev)
    dir_rows = (pl.ds(0, half), pl.ds(half, half))
    subs = (pl.ds(0, sub), pl.ds(sub, sub))

    def rs_copy(dr, s, u):
        return pltpu.make_async_remote_copy(
            src_ref=sbuf.at[dr, s, :, subs[u]], dst_ref=rbuf.at[dr, s, :, subs[u]],
            send_sem=rs_send.at[dr, s, u], recv_sem=rs_recv.at[dr, s, u],
            device_id={'tp': targets[dr]}, device_id_type=MESH)

    def ag_copy(dr, a, u, idx):
        ref = out_v.at[dir_rows[dr], pl.ds(pl.multiple_of(idx * chunk + u * sub, HEAD), sub)]
        return pltpu.make_async_remote_copy(
            src_ref=ref, dst_ref=ref, send_sem=ag_send.at[dr, a, u], recv_sem=ag_recv.at[dr, a, u],
            device_id={'tp': targets[dr]}, device_id_type=MESH)

    order = (y_prev, y_next, lax.rem(ty + 2, tp_n), ty)
    for i in range(tp_n):
        cols = pl.ds(pl.multiple_of(order[i] * chunk, HEAD), chunk)
        part = jnp.dot(o_v[...], wo_v[:, cols], preferred_element_type=F32)
        part_v[i] = part
        if i < 2:
            sbuf[i, 0] = part[i * half:(i + 1) * half].astype(BF16)
            for u in range(2):
                rs_copy(i, 0, u).start()

    use = ((2, 1), (2, 0))
    for s in (1, 2):
        for u in range(2):
            for dr in range(2):
                rs_copy(dr, s - 1, u).wait_recv()
                got = rbuf[dr, s - 1, :, subs[u]].astype(F32)
                sbuf[dr, s, :, subs[u]] = (got + part_v[use[dr][s - 1], dir_rows[dr], subs[u]]).astype(BF16)
                rs_copy(dr, s, u).start()

    for u in range(2):
        for dr in range(2):
            rs_copy(dr, 2, u).wait_recv()
            cols = pl.ds(pl.multiple_of(ty * chunk + u * sub, HEAD), sub)
            a_sum = rbuf[dr, 2, :, subs[u]].astype(F32) + part_v[3, dir_rows[dr], subs[u]]
            out_v[dir_rows[dr], cols] = (x_v[dir_rows[dr], cols].astype(F32) + a_sum).astype(BF16)
            ag_copy(dr, 0, u, ty).start()

    def held(dr, a):
        return lax.rem(ty + tp_n - a, tp_n) if dr == 0 else lax.rem(ty + a, tp_n)

    for a in range(1, tp_n):
        for u in range(2):
            for dr in range(2):
                idx = held(dr, a)
                ag_copy(dr, a - 1, u, idx).wait_recv()
                if a < tp_n - 1:
                    ag_copy(dr, a, u, idx).start()

    k_out[...] = jnp.stack([kv_v[i, 0, own_rows, :] for i in range(kv_heads)], axis=1)
    v_out[...] = jnp.stack([kv_v[i, 1, own_rows, :] for i in range(kv_heads)], axis=1)

    for a in range(tp_n - 1):
        for u in range(2):
            for dr in range(2):
                rs_copy(dr, a, u).wait_send()
                ag_copy(dr, a, u, held(dr, a)).wait_send()
    for frm in range(chips):
        @pl.when(chip == frm)
        def _(frm=frm):
            for h in range(kv_heads):
                for a, to, hs, slot in plan:
                    if a == frm and h in hs:
                        own_copy(to, h, slot).wait_send()

    @pl.when(core == 0)
    def _():
        for h in range(kv_heads):
            sib_copy(h).wait_send()

    @pl.when(chip == 0)
    def _():
        kv_copy(1, at_chip(1), at_chip(3), relay_send.at[0], kv_recv.at[1, 1]).wait_send()

    @pl.when(chip == 2)
    def _():
        kv_copy(0, at_chip(1), at_chip(3), relay_send.at[0], kv_recv.at[1, 0]).wait_send()

    @pl.when(chip == 3)
    def _():
        for h in range(kv_heads):
            kv_copy(h, at_chip(0), at_chip(2), relay_send.at[h], kv_recv.at[0, h]).wait_send()
    for t in range(chips - 1):
        @pl.when(t < chip)
        def _(t=t):
            for h in range(kv_heads):
                kv_copy(h, at_chip(t), sibling, fwd_send.at[t, h], fwd_recv.at[t, h]).wait_send()


def solution(mesh):
    tp_n = mesh.shape['tp']
    cp_n = mesh.shape['cp']
    row_spec = P(('dp', 'cp'), None)
    cache_spec = P(('dp', 'cp'), 'tp', None)
    head_cols = P(None, 'tp')

    def local_block(hidden, positions, norm_gain, w_query, w_key, w_value, w_out):
        rows, width = hidden.shape
        q_cols = w_query.shape[1]
        kv_cols = w_key.shape[1]
        heads = q_cols // HEAD
        kv_heads = kv_cols // HEAD
        chunk = width // tp_n
        half = rows // 2
        any_spec = pl.BlockSpec(memory_space=pl.ANY)
        vmem_spec = pl.BlockSpec(memory_space=pltpu.VMEM)
        dma = pltpu.SemaphoreType.DMA
        chips = cp_n // 2
        out, k_cache, v_cache = pl.pallas_call(
            functools.partial(block_kernel, tp_n, cp_n),
            out_shape=(pltpu.VMEM((rows, width), BF16),
                       pltpu.VMEM((rows, kv_heads, HEAD), BF16),
                       pltpu.VMEM((rows, kv_heads, HEAD), BF16)),
            in_specs=[any_spec, vmem_spec, vmem_spec, any_spec, any_spec, any_spec, any_spec],
            out_specs=(vmem_spec, vmem_spec, vmem_spec),
            scratch_shapes=[
                pltpu.VMEM((rows, width), BF16),
                pltpu.VMEM((rows, width), BF16),
                pltpu.VMEM((width, 2 * kv_cols), BF16),
                pltpu.VMEM((width, q_cols), BF16),
                pltpu.VMEM((q_cols, width), BF16),
                pltpu.VMEM((1, width), F32),
                pltpu.VMEM((rows, HEAD), F32),
                pltpu.VMEM((rows, HEAD), F32),
                pltpu.VMEM((heads, rows, HEAD), BF16),
                pltpu.VMEM((kv_heads, 2, cp_n * rows, HEAD), BF16),
                pltpu.VMEM((heads, rows, HEAD), F32),
                pltpu.VMEM((heads, rows, HEAD), F32),
                pltpu.VMEM((heads, rows, HEAD), F32),
                pltpu.VMEM((rows, q_cols), BF16),
                pltpu.VMEM((tp_n, rows, chunk), F32),
                pltpu.VMEM((2, tp_n - 1, half, chunk), BF16),
                pltpu.VMEM((2, tp_n - 1, half, chunk), BF16),
                dma, dma((2,)), dma((2,)), dma,
                dma((2, kv_heads)), dma((kv_heads,)), dma((chips, kv_heads)), dma((chips, kv_heads)), dma((chips, kv_heads)),
                dma((2, tp_n - 1, 2)), dma((2, tp_n - 1, 2)), dma((2, tp_n - 1, 2)), dma((2, tp_n - 1, 2)),
            ],
            compiler_params=pltpu.CompilerParams(collective_id=0, has_side_effects=True, vmem_limit_bytes=VMEM_LIMIT),
        )(hidden, positions.reshape(1, rows), norm_gain.reshape(width // HEAD, HEAD), w_query, w_key, w_value, w_out)
        return out, k_cache, v_cache

    return jax.shard_map(local_block, mesh=mesh, in_specs=(row_spec, P(('dp', 'cp')), P(None), head_cols, head_cols, head_cols, P('tp', None)), out_specs=(row_spec, cache_spec, cache_spec), check_vma=False)
```

```python
import math
import functools
import jax
import jax.numpy as jnp
from jax import lax
from jax.experimental import pallas as pl
from jax.experimental.pallas import tpu as pltpu
from jax.sharding import PartitionSpec as P

HEAD = 128
EPS = 1e-5
LOG_THETA = math.log(1000000.0)
EXP2_SCALE = math.log2(math.e) / math.sqrt(HEAD)
MESH = pl.DeviceIdType.MESH
F32 = jnp.float32
BF16 = jnp.bfloat16
UNROLL = 4
X_STRIPS = 4
KV_STRIPS = 2
Q_STRIPS = 2
NORM_ROWS = 64
VMEM_LIMIT = 56 * 1024 * 1024


def block_kernel(tp_n, cp_n, x_hbm, pos_ref, gain_ref, wq_hbm, wk_hbm, wv_hbm, wo_hbm,
                 out_v, k_out, v_out,
                 x_v, h_v, wkv_v, wq_v, wo_v, gain_v, cos_v, sin_v, q_v, kv_v, m_v, l_v, acc_v, o_v,
                 part_v, sbuf, rbuf, kv_acc,
                 x_sem, wkv_sem, wq_sem, wo_sem,
                 own_send, relay_send, fwd_send, kv_recv, fwd_recv,
                 rs_send, rs_recv, ag_send, ag_recv):
    rows, width = x_v.shape
    chips = cp_n // 2
    heads = q_v.shape[0]
    kv_heads = kv_v.shape[0]
    group = heads // kv_heads
    half = rows // 2
    chunk = width // tp_n
    sub = chunk // 2
    ty = lax.axis_index('tp')
    c_me = lax.axis_index('cp')
    chip = c_me // 2
    core = lax.rem(c_me, 2)
    sibling = chip * 2 + (1 - core)

    strip = rows // X_STRIPS
    depth = width // KV_STRIPS
    kvw = kv_heads * HEAD
    qw = wq_v.shape[1] // Q_STRIPS
    x_copies = [pltpu.make_async_copy(x_hbm.at[pl.ds(i * strip, strip)], x_v.at[pl.ds(i * strip, strip)], x_sem.at[i])
                for i in range(X_STRIPS)]
    wkv_copies = [[pltpu.make_async_copy(w_hbm.at[pl.ds(i * depth, depth)],
                                         wkv_v.at[pl.ds(i * depth, depth), pl.ds(n * kvw, kvw)], wkv_sem.at[n, i])
                   for n, w_hbm in enumerate((wk_hbm, wv_hbm))] for i in range(KV_STRIPS)]
    wq_copies = [pltpu.make_async_copy(wq_hbm.at[:, pl.ds(j * qw, qw)], wq_v.at[:, pl.ds(j * qw, qw)], wq_sem.at[j])
                 for j in range(Q_STRIPS)]
    wo_copy = pltpu.make_async_copy(wo_hbm, wo_v, wo_sem)
    for cp in x_copies:
        cp.start()
    for cp in wkv_copies[0]:
        cp.start()

    barrier = pltpu.get_barrier_semaphore()
    y_next = lax.rem(ty + 1, tp_n)
    y_prev = lax.rem(ty + tp_n - 1, tp_n)
    partners = [{'tp': y_next}, {'tp': y_prev}, {'cp': sibling}]
    for d in range(1, chips):
        partners.append({'cp': lax.rem(c_me + 2 * d, cp_n)})
    for dev in partners:
        pl.semaphore_signal(barrier, inc=1, device_id=dev, device_id_type=MESH)

    freq = jnp.exp(lax.broadcasted_iota(jnp.int32, (HEAD // 2, rows), 0).astype(F32) * (-2.0 * LOG_THETA / HEAD))
    angles = pos_ref[...].astype(F32) * freq
    cos_t = jnp.cos(angles)
    sin_t = jnp.sin(angles)
    cos_v[...] = jnp.concatenate([cos_t, cos_t], axis=0).T
    sin_v[...] = jnp.concatenate([-sin_t, sin_t], axis=0).T

    gain_f = gain_ref[...].astype(F32)
    for i in range(width // HEAD):
        gain_v[:, i * HEAD:(i + 1) * HEAD] = gain_f[i:i + 1, :]

    for i in range(X_STRIPS):
        x_copies[i].wait()

        def norm_rows(n, carry, i=i):
            r = pl.ds(pl.multiple_of(i * strip + n * NORM_ROWS, NORM_ROWS), NORM_ROWS)
            xf = x_v[r, :].astype(F32)
            inv = lax.rsqrt(jnp.mean(xf * xf, axis=-1, keepdims=True) + EPS)
            h_v[r, :] = (xf * inv * gain_v[...]).astype(BF16)
            return carry
        lax.fori_loop(0, strip // NORM_ROWS, norm_rows, 0)
        if i == 0:
            for pair in wkv_copies[1:]:
                for cp in pair:
                    cp.start()
        if i == X_STRIPS - 1:
            for cp in wq_copies:
                cp.start()

    def rope(t):
        return t * cos_v[...] + pltpu.roll(t, HEAD // 2, 1) * sin_v[...]

    for i in range(KV_STRIPS):
        for cp in wkv_copies[i]:
            cp.wait()
        part_kv = jnp.dot(h_v[:, i * depth:(i + 1) * depth], wkv_v[i * depth:(i + 1) * depth, :], preferred_element_type=F32)
        if i == 0:
            kv_acc[...] = part_kv
        else:
            kv_acc[...] += part_kv
    kv_f = kv_acc[...]

    def kv_rows(c):
        return pl.ds(pl.multiple_of(c * rows, rows), rows)

    own_rows = kv_rows(c_me)
    for i in range(kv_heads):
        k_h = rope(kv_f[:, i * HEAD:(i + 1) * HEAD]).astype(BF16)
        kv_v[i, 0, own_rows, :] = k_h
        v_h = kv_f[:, kvw + i * HEAD:kvw + (i + 1) * HEAD].astype(BF16)
        kv_v[i, 1, own_rows, :] = v_h

    pl.semaphore_wait(barrier, len(partners))

    def kv_copy(h, src_c, target_c, ssem, rsem):
        ref = kv_v.at[h, :, kv_rows(src_c), :]
        return pltpu.make_async_remote_copy(src_ref=ref, dst_ref=ref, send_sem=ssem, recv_sem=rsem,
                                            device_id={'cp': target_c}, device_id_type=MESH)

    def at_chip(i):
        return i * 2 + core

    plan = ((0, 3, (0, 1), 0), (0, 1, (0, 1), 1), (1, 0, (1,), 0), (1, 2, (0, 1), 1), (2, 3, (0, 1), 1))

    def own_copy(to, h, slot):
        return kv_copy(h, c_me, at_chip(to), own_send.at[slot, h], kv_recv.at[chip, h])

    def sib_copy(h):
        return kv_copy(h, c_me, sibling, fwd_send.at[chip, h], fwd_recv.at[chip, h])

    for frm in range(chips):
        @pl.when(chip == frm)
        def _(frm=frm):
            for h in range(kv_heads):
                for a, to, hs, slot in plan:
                    if a == frm and h in hs:
                        own_copy(to, h, slot).start()

    @pl.when(core == 0)
    def _():
        for h in range(kv_heads):
            sib_copy(h).start()

    for j in range(Q_STRIPS):
        wq_copies[j].wait()
        if j == Q_STRIPS - 1:
            wo_copy.start()
        q_f = jnp.dot(h_v[...], wq_v[:, j * qw:(j + 1) * qw], preferred_element_type=F32)
        for i in range(qw // HEAD):
            q_v[j * (qw // HEAD) + i] = rope(q_f[:, i * HEAD:(i + 1) * HEAD]).astype(BF16)

    def fold(p):
        out = p[:, 0:HEAD]
        for i in range(1, p.shape[1] // HEAD):
            out = out + p[:, i * HEAD:(i + 1) * HEAD]
        return out

    def scores(hd, kh, keys):
        return lax.dot_general(q_v[hd], kv_v[kh, 0, keys, :], (((1,), (1,)), ((), ())), preferred_element_type=F32)

    def own_heads(i, carry):
        hds = [i * UNROLL + u for u in range(UNROLL)]
        kh = hds[0] // group
        ss = [scores(hd, kh, own_rows) for hd in hds]
        r_i = lax.broadcasted_iota(jnp.int32, (rows, rows), 0)
        c_i = lax.broadcasted_iota(jnp.int32, (rows, rows), 1)
        ss = [jnp.where(c_i <= r_i, s, -jnp.inf) for s in ss]
        ms = [jnp.max(s, axis=1, keepdims=True) for s in ss]
        ps = [jnp.exp2((s - m) * EXP2_SCALE) for s, m in zip(ss, ms)]
        vals = kv_v[kh, 1, own_rows, :]
        accs = [jnp.dot(p.astype(BF16), vals, preferred_element_type=F32) for p in ps]
        for hd, m, p, acc in zip(hds, ms, ps, accs):
            m_v[hd] = jnp.broadcast_to(m, (rows, HEAD))
            l_v[hd] = fold(p)
            acc_v[hd] = acc
        return carry
    lax.fori_loop(0, heads // UNROLL, own_heads, 0)

    def attend(start, count, kh):
        keys = pl.ds(pl.multiple_of(start, rows), count)

        def some_heads(i, carry):
            hds = [kh * group + i * UNROLL + u for u in range(UNROLL)]
            ss = [scores(hd, kh, keys) for hd in hds]
            olds = [m_v[hd] for hd in hds]
            ls = [l_v[hd] for hd in hds]
            accs = [acc_v[hd] for hd in hds]
            news = [jnp.maximum(m, jnp.max(s, axis=1, keepdims=True)) for m, s in zip(olds, ss)]
            alphas = [jnp.exp2((m - n) * EXP2_SCALE) for m, n in zip(olds, news)]
            ps = [jnp.exp2((s - n[:, 0:1]) * EXP2_SCALE) for s, n in zip(ss, news)]
            vals = kv_v[kh, 1, keys, :]
            pvs = [jnp.dot(p.astype(BF16), vals, preferred_element_type=F32) for p in ps]
            for hd, n, l, a, p, acc, pv in zip(hds, news, ls, alphas, ps, accs, pvs):
                m_v[hd] = n
                l_v[hd] = l * a + fold(p)
                acc_v[hd] = acc * a + pv
            return carry
        lax.fori_loop(0, group // UNROLL, some_heads, 0)

    def sib_wait(i, h):
        kv_copy(h, 2 * i + 1 - core, c_me, fwd_send.at[i, h], fwd_recv.at[i, h]).wait_recv()

    @pl.when(chip == 0)
    def _():
        kv_copy(1, at_chip(1), c_me, relay_send.at[0], kv_recv.at[1, 1]).wait_recv()
        kv_copy(1, at_chip(1), at_chip(3), relay_send.at[0], kv_recv.at[1, 1]).start()

    @pl.when(core == 1)
    def _():
        for h in range(kv_heads):
            sib_wait(chip, h)
            attend(sibling * rows, rows, h)

    def source(t):
        return lax.rem(chip - 1 + chip // 3 - t + 3, 3)

    def take(t, h):
        src = source(t)
        kv_copy(h, at_chip(src), c_me, own_send.at[0, h], kv_recv.at[src, h]).wait_recv()
        if t == 0:
            @pl.when(chip == 1)
            def _():
                kv_copy(h, at_chip(0), at_chip(2), relay_send.at[h], kv_recv.at[0, h]).start()
            if h == 0:
                @pl.when(chip == 2)
                def _():
                    kv_copy(h, at_chip(1), at_chip(3), relay_send.at[0], kv_recv.at[1, h]).start()
        kv_copy(h, at_chip(src), sibling, fwd_send.at[src, h], fwd_recv.at[src, h]).start()

    def use_block(t, h):
        src = source(t)
        sib_wait(src, h)
        attend(src * 2 * rows, 2 * rows, h)

    @pl.when(chip == 3)
    def _():
        take(0, 0)
        take(1, 0)
        use_block(0, 0)
        take(0, 1)
        take(1, 1)
        use_block(1, 0)
        use_block(0, 1)
        take(2, 0)
        take(2, 1)
        use_block(1, 1)
        use_block(2, 0)
        use_block(2, 1)

    @pl.when((chip == 1) | (chip == 2))
    def _():
        take(0, 0)
        take(0, 1)
        use_block(0, 0)

    @pl.when(chip == 1)
    def _():
        use_block(0, 1)

    @pl.when(chip == 2)
    def _():
        take(1, 0)
        use_block(0, 1)
        take(1, 1)
        use_block(1, 0)
        use_block(1, 1)

    def finish_head(hd, carry):
        total = jnp.sum(l_v[hd], axis=1, keepdims=True)
        o_v[:, pl.ds(pl.multiple_of(hd * HEAD, HEAD), HEAD)] = (acc_v[hd] / total).astype(BF16)
        return carry
    lax.fori_loop(0, heads, finish_head, 0)

    wo_copy.wait()
    targets = (y_next, y_prev)
    dir_rows = (pl.ds(0, half), pl.ds(half, half))
    subs = (pl.ds(0, sub), pl.ds(sub, sub))

    def rs_copy(dr, s, u):
        return pltpu.make_async_remote_copy(
            src_ref=sbuf.at[dr, s, :, subs[u]], dst_ref=rbuf.at[dr, s, :, subs[u]],
            send_sem=rs_send.at[dr, s, u], recv_sem=rs_recv.at[dr, s, u],
            device_id={'tp': targets[dr]}, device_id_type=MESH)

    def ag_copy(dr, a, u, idx):
        ref = out_v.at[dir_rows[dr], pl.ds(pl.multiple_of(idx * chunk + u * sub, HEAD), sub)]
        return pltpu.make_async_remote_copy(
            src_ref=ref, dst_ref=ref, send_sem=ag_send.at[dr, a, u], recv_sem=ag_recv.at[dr, a, u],
            device_id={'tp': targets[dr]}, device_id_type=MESH)

    order = (y_prev, y_next, lax.rem(ty + 2, tp_n), ty)
    def project(i, r):
        cols = pl.ds(pl.multiple_of(order[i] * chunk, HEAD), chunk)
        return jnp.dot(o_v[r, :], wo_v[:, cols], preferred_element_type=F32)

    for dr in range(2):
        sbuf[dr, 0] = project(dr, dir_rows[dr]).astype(BF16)
        for u in range(2):
            rs_copy(dr, 0, u).start()
    for i in (2, 0, 1, 3):
        r = pl.ds(0, rows) if i > 1 else dir_rows[1 - i]
        part_v[i, r, :] = project(i, r)

    k_out[...] = jnp.stack([kv_v[i, 0, own_rows, :] for i in range(kv_heads)], axis=1)
    v_out[...] = jnp.stack([kv_v[i, 1, own_rows, :] for i in range(kv_heads)], axis=1)

    use = ((2, 1), (2, 0))
    for s in (1, 2):
        for u in range(2):
            for dr in range(2):
                rs_copy(dr, s - 1, u).wait_recv()
                got = rbuf[dr, s - 1, :, subs[u]].astype(F32)
                sbuf[dr, s, :, subs[u]] = (got + part_v[use[dr][s - 1], dir_rows[dr], subs[u]]).astype(BF16)
                rs_copy(dr, s, u).start()

    for u in range(2):
        for dr in range(2):
            rs_copy(dr, 2, u).wait_recv()
            cols = pl.ds(pl.multiple_of(ty * chunk + u * sub, HEAD), sub)
            a_sum = rbuf[dr, 2, :, subs[u]].astype(F32) + part_v[3, dir_rows[dr], subs[u]]
            out_v[dir_rows[dr], cols] = (x_v[dir_rows[dr], cols].astype(F32) + a_sum).astype(BF16)
            ag_copy(dr, 0, u, ty).start()

    def held(dr, a):
        return lax.rem(ty + tp_n - a, tp_n) if dr == 0 else lax.rem(ty + a, tp_n)

    for a in range(1, tp_n):
        for u in range(2):
            for dr in range(2):
                idx = held(dr, a)
                ag_copy(dr, a - 1, u, idx).wait_recv()
                if a < tp_n - 1:
                    ag_copy(dr, a, u, idx).start()

    for a in range(tp_n - 1):
        for u in range(2):
            for dr in range(2):
                rs_copy(dr, a, u).wait_send()
                ag_copy(dr, a, u, held(dr, a)).wait_send()
    for frm in range(chips):
        @pl.when(chip == frm)
        def _(frm=frm):
            for h in range(kv_heads):
                for a, to, hs, slot in plan:
                    if a == frm and h in hs:
                        own_copy(to, h, slot).wait_send()

    @pl.when(core == 0)
    def _():
        for h in range(kv_heads):
            sib_copy(h).wait_send()

    @pl.when(chip == 0)
    def _():
        kv_copy(1, at_chip(1), at_chip(3), relay_send.at[0], kv_recv.at[1, 1]).wait_send()

    @pl.when(chip == 2)
    def _():
        kv_copy(0, at_chip(1), at_chip(3), relay_send.at[0], kv_recv.at[1, 0]).wait_send()

    @pl.when(chip == 1)
    def _():
        for h in range(kv_heads):
            kv_copy(h, at_chip(0), at_chip(2), relay_send.at[h], kv_recv.at[0, h]).wait_send()
    for t in range(chips - 1):
        @pl.when(t < chip)
        def _(t=t):
            for h in range(kv_heads):
                kv_copy(h, at_chip(t), sibling, fwd_send.at[t, h], fwd_recv.at[t, h]).wait_send()


def store_kernel(out_v, k_v, v_v, out_hbm, k_hbm, v_hbm, sem):
    pairs = ((k_v, k_hbm), (v_v, v_hbm), (out_v, out_hbm))
    copies = [pltpu.make_async_copy(src, dst, sem.at[i]) for i, (src, dst) in enumerate(pairs)]
    for cp in copies:
        cp.start()
    for cp in copies:
        cp.wait()


def solution(mesh):
    tp_n = mesh.shape['tp']
    cp_n = mesh.shape['cp']
    row_spec = P(('dp', 'cp'), None)
    cache_spec = P(('dp', 'cp'), 'tp', None)
    head_cols = P(None, 'tp')

    def local_block(hidden, positions, norm_gain, w_query, w_key, w_value, w_out):
        rows, width = hidden.shape
        q_cols = w_query.shape[1]
        kv_cols = w_key.shape[1]
        heads = q_cols // HEAD
        kv_heads = kv_cols // HEAD
        chunk = width // tp_n
        half = rows // 2
        any_spec = pl.BlockSpec(memory_space=pl.ANY)
        vmem_spec = pl.BlockSpec(memory_space=pltpu.VMEM)
        dma = pltpu.SemaphoreType.DMA
        chips = cp_n // 2
        out, k_cache, v_cache = pl.pallas_call(
            functools.partial(block_kernel, tp_n, cp_n),
            out_shape=(pltpu.VMEM((rows, width), BF16),
                       pltpu.VMEM((rows, kv_heads, HEAD), BF16),
                       pltpu.VMEM((rows, kv_heads, HEAD), BF16)),
            in_specs=[any_spec, vmem_spec, vmem_spec, any_spec, any_spec, any_spec, any_spec],
            out_specs=(vmem_spec, vmem_spec, vmem_spec),
            scratch_shapes=[
                pltpu.VMEM((rows, width), BF16),
                pltpu.VMEM((rows, width), BF16),
                pltpu.VMEM((width, 2 * kv_cols), BF16),
                pltpu.VMEM((width, q_cols), BF16),
                pltpu.VMEM((q_cols, width), BF16),
                pltpu.VMEM((1, width), F32),
                pltpu.VMEM((rows, HEAD), F32),
                pltpu.VMEM((rows, HEAD), F32),
                pltpu.VMEM((heads, rows, HEAD), BF16),
                pltpu.VMEM((kv_heads, 2, cp_n * rows, HEAD), BF16),
                pltpu.VMEM((heads, rows, HEAD), F32),
                pltpu.VMEM((heads, rows, HEAD), F32),
                pltpu.VMEM((heads, rows, HEAD), F32),
                pltpu.VMEM((rows, q_cols), BF16),
                pltpu.VMEM((tp_n, rows, chunk), F32),
                pltpu.VMEM((2, tp_n - 1, half, chunk), BF16),
                pltpu.VMEM((2, tp_n - 1, half, chunk), BF16),
                pltpu.VMEM((rows, 2 * kv_cols), F32),
                dma((X_STRIPS,)), dma((2, KV_STRIPS)), dma((Q_STRIPS,)), dma,
                dma((2, kv_heads)), dma((kv_heads,)), dma((chips, kv_heads)), dma((chips, kv_heads)), dma((chips, kv_heads)),
                dma((2, tp_n - 1, 2)), dma((2, tp_n - 1, 2)), dma((2, tp_n - 1, 2)), dma((2, tp_n - 1, 2)),
            ],
            compiler_params=pltpu.CompilerParams(collective_id=0, has_side_effects=True, vmem_limit_bytes=VMEM_LIMIT),
        )(hidden, positions.reshape(1, rows), norm_gain.reshape(width // HEAD, HEAD), w_query, w_key, w_value, w_out)
        results = (out, k_cache, v_cache)
        return pl.pallas_call(
            store_kernel,
            out_shape=tuple(jax.ShapeDtypeStruct(r.shape, BF16) for r in results),
            in_specs=[vmem_spec] * 3,
            out_specs=(any_spec,) * 3,
            scratch_shapes=[dma((3,))],
        )(*[pltpu.with_memory_space_constraint(r, pltpu.VMEM) for r in results])

    return jax.shard_map(local_block, mesh=mesh, in_specs=(row_spec, P(('dp', 'cp')), P(None), head_cols, head_cols, head_cols, P('tp', None)), out_specs=(row_spec, cache_spec, cache_spec), check_vma=False)
```

```python
import math
import functools
import jax
import jax.numpy as jnp
from jax import lax
from jax.experimental import pallas as pl
from jax.experimental.pallas import tpu as pltpu
from jax.sharding import PartitionSpec as P

HEAD = 128
EPS = 1e-5
LOG_THETA = math.log(1000000.0)
EXP2_SCALE = math.log2(math.e) / math.sqrt(HEAD)
MESH = pl.DeviceIdType.MESH
F32 = jnp.float32
BF16 = jnp.bfloat16
MERGE = 4
X_STRIPS = 4
KV_STRIPS = 2
Q_STRIPS = 2
NORM_ROWS = 64
VMEM_LIMIT = 56 * 1024 * 1024


def block_kernel(tp_n, cp_n, x_hbm, pos_ref, gain_ref, wq_hbm, wk_hbm, wv_hbm, wo_hbm,
                 out_v, k_out, v_out,
                 x_v, h_v, wkv_v, wq_v, wo_v, gain_v, cos_v, sin_v, q_v, kv_v, m_v, l_v, acc_v, o_v,
                 part_v, sbuf, rbuf, kv_acc,
                 x_sem, wkv_sem, wq_sem, wo_sem,
                 own_send, relay_send, fwd_send, kv_recv, fwd_recv,
                 rs_send, rs_recv, ag_send, ag_recv):
    rows, width = x_v.shape
    chips = cp_n // 2
    heads = q_v.shape[0]
    kv_heads = kv_v.shape[0]
    group = heads // kv_heads
    half = rows // 2
    chunk = width // tp_n
    sub = chunk // 2
    ty = lax.axis_index('tp')
    c_me = lax.axis_index('cp')
    chip = c_me // 2
    core = lax.rem(c_me, 2)
    sibling = chip * 2 + (1 - core)

    strip = rows // X_STRIPS
    depth = width // KV_STRIPS
    kvw = kv_heads * HEAD
    qw = wq_v.shape[1] // Q_STRIPS
    x_copies = [pltpu.make_async_copy(x_hbm.at[pl.ds(i * strip, strip)], x_v.at[pl.ds(i * strip, strip)], x_sem.at[i])
                for i in range(X_STRIPS)]
    wkv_copies = [[pltpu.make_async_copy(w_hbm.at[pl.ds(i * depth, depth)],
                                         wkv_v.at[pl.ds(i * depth, depth), pl.ds(n * kvw, kvw)], wkv_sem.at[n, i])
                   for n, w_hbm in enumerate((wk_hbm, wv_hbm))] for i in range(KV_STRIPS)]
    wq_copies = [pltpu.make_async_copy(wq_hbm.at[:, pl.ds(j * qw, qw)], wq_v.at[:, pl.ds(j * qw, qw)], wq_sem.at[j])
                 for j in range(Q_STRIPS)]
    wo_copy = pltpu.make_async_copy(wo_hbm, wo_v, wo_sem)
    for cp in x_copies:
        cp.start()
    for cp in wkv_copies[0]:
        cp.start()

    barrier = pltpu.get_barrier_semaphore()
    y_next = lax.rem(ty + 1, tp_n)
    y_prev = lax.rem(ty + tp_n - 1, tp_n)
    partners = [{'tp': y_next}, {'tp': y_prev}, {'cp': sibling}]
    for d in range(1, chips):
        partners.append({'cp': lax.rem(c_me + 2 * d, cp_n)})
    for dev in partners:
        pl.semaphore_signal(barrier, inc=1, device_id=dev, device_id_type=MESH)

    freq = jnp.exp(lax.broadcasted_iota(jnp.int32, (HEAD // 2, rows), 0).astype(F32) * (-2.0 * LOG_THETA / HEAD))
    angles = pos_ref[...].astype(F32) * freq
    cos_t = jnp.cos(angles)
    sin_t = jnp.sin(angles)
    cos_v[...] = jnp.concatenate([cos_t, cos_t], axis=0).T
    sin_v[...] = jnp.concatenate([-sin_t, sin_t], axis=0).T

    gain_f = gain_ref[...].astype(F32)
    for i in range(width // HEAD):
        gain_v[:, i * HEAD:(i + 1) * HEAD] = gain_f[i:i + 1, :]

    for i in range(X_STRIPS):
        x_copies[i].wait()

        def norm_rows(n, carry, i=i):
            r = pl.ds(pl.multiple_of(i * strip + n * NORM_ROWS, NORM_ROWS), NORM_ROWS)
            xf = x_v[r, :].astype(F32)
            inv = lax.rsqrt(jnp.mean(xf * xf, axis=-1, keepdims=True) + EPS)
            h_v[r, :] = (xf * inv * gain_v[...]).astype(BF16)
            return carry
        lax.fori_loop(0, strip // NORM_ROWS, norm_rows, 0)
        if i == 0:
            for pair in wkv_copies[1:]:
                for cp in pair:
                    cp.start()
        if i == X_STRIPS - 1:
            for cp in wq_copies:
                cp.start()

    def rope(t):
        return t * cos_v[...] + pltpu.roll(t, HEAD // 2, 1) * sin_v[...]

    for i in range(KV_STRIPS):
        for cp in wkv_copies[i]:
            cp.wait()
        part_kv = jnp.dot(h_v[:, i * depth:(i + 1) * depth], wkv_v[i * depth:(i + 1) * depth, :], preferred_element_type=F32)
        if i == 0:
            kv_acc[...] = part_kv
        else:
            kv_acc[...] += part_kv
    kv_f = kv_acc[...]

    def kv_rows(c):
        return pl.ds(pl.multiple_of(c * rows, rows), rows)

    own_rows = kv_rows(c_me)
    for i in range(kv_heads):
        k_h = rope(kv_f[:, i * HEAD:(i + 1) * HEAD]).astype(BF16)
        kv_v[i, 0, own_rows, :] = k_h
        v_h = kv_f[:, kvw + i * HEAD:kvw + (i + 1) * HEAD].astype(BF16)
        kv_v[i, 1, own_rows, :] = v_h

    pl.semaphore_wait(barrier, len(partners))

    def kv_copy(h, src_c, target_c, ssem, rsem):
        ref = kv_v.at[h, :, kv_rows(src_c), :]
        return pltpu.make_async_remote_copy(src_ref=ref, dst_ref=ref, send_sem=ssem, recv_sem=rsem,
                                            device_id={'cp': target_c}, device_id_type=MESH)

    def at_chip(i):
        return i * 2 + core

    plan = ((0, 3, 1, 0), (0, 1, 0, 1), (0, 3, 0, 0), (0, 1, 1, 1), (1, 0, 1, 0), (1, 2, 0, 1), (1, 2, 1, 1), (2, 3, 1, 1), (2, 3, 0, 1))

    def own_copy(to, h, slot):
        return kv_copy(h, c_me, at_chip(to), own_send.at[slot, h], kv_recv.at[chip, h])

    def sib_copy(h):
        return kv_copy(h, c_me, sibling, fwd_send.at[chip, h], fwd_recv.at[chip, h])

    for frm in range(chips):
        @pl.when(chip == frm)
        def _(frm=frm):
            for a, to, h, slot in plan:
                if a == frm:
                    own_copy(to, h, slot).start()

    @pl.when(core == 0)
    def _():
        for h in range(kv_heads):
            sib_copy(h).start()

    for j in range(Q_STRIPS):
        wq_copies[j].wait()
        if j == Q_STRIPS - 1:
            wo_copy.start()
        q_f = jnp.dot(h_v[...], wq_v[:, j * qw:(j + 1) * qw], preferred_element_type=F32)
        for i in range(qw // HEAD):
            q_v[j * (qw // HEAD) + i] = rope(q_f[:, i * HEAD:(i + 1) * HEAD]).astype(BF16)

    span = MERGE * rows

    def merged(ref, hd):
        return ref[pl.ds(hd, MERGE)].reshape(span, HEAD)

    def put(ref, hd, val):
        ref[pl.ds(hd, MERGE)] = val.reshape(MERGE, rows, HEAD)

    def tiles(s):
        return [s[:, i * HEAD:(i + 1) * HEAD] for i in range(s.shape[1] // HEAD)]

    def scores(hd, kh, keys):
        return lax.dot_general(merged(q_v, hd), kv_v[kh, 0, keys, :], (((1,), (1,)), ((), ())), preferred_element_type=F32)

    def row_max(s):
        return jnp.broadcast_to(jnp.max(functools.reduce(jnp.maximum, tiles(s)), axis=1, keepdims=True), (span, HEAD))

    def own_heads(i, carry):
        hd = i * MERGE
        kh = hd // group
        s = scores(hd, kh, own_rows)
        r_i = lax.rem(lax.broadcasted_iota(jnp.int32, (span, rows), 0), rows)
        c_i = lax.broadcasted_iota(jnp.int32, (span, rows), 1)
        s = jnp.where(c_i <= r_i, s, -jnp.inf)
        m = row_max(s)
        ps = [jnp.exp2((t - m) * EXP2_SCALE) for t in tiles(s)]
        p = jnp.concatenate([t.astype(BF16) for t in ps], axis=1)
        put(m_v, hd, m)
        put(l_v, hd, functools.reduce(jnp.add, ps))
        put(acc_v, hd, jnp.dot(p, kv_v[kh, 1, own_rows, :], preferred_element_type=F32))
        return carry
    lax.fori_loop(0, heads // MERGE, own_heads, 0)

    def attend(start, count, kh):
        keys = pl.ds(pl.multiple_of(start, rows), count)

        def some_heads(i, carry):
            hd = kh * group + i * MERGE
            s = scores(hd, kh, keys)
            old = merged(m_v, hd)
            new = jnp.maximum(old, row_max(s))
            alpha = jnp.exp2((old - new) * EXP2_SCALE)
            ps = [jnp.exp2((t - new) * EXP2_SCALE) for t in tiles(s)]
            p = jnp.concatenate([t.astype(BF16) for t in ps], axis=1)
            put(m_v, hd, new)
            put(l_v, hd, merged(l_v, hd) * alpha + functools.reduce(jnp.add, ps))
            put(acc_v, hd, merged(acc_v, hd) * alpha + jnp.dot(p, kv_v[kh, 1, keys, :], preferred_element_type=F32))
            return carry
        lax.fori_loop(0, group // MERGE, some_heads, 0)

    def sib_wait(i, h):
        kv_copy(h, 2 * i + 1 - core, c_me, fwd_send.at[i, h], fwd_recv.at[i, h]).wait_recv()

    @pl.when(chip == 0)
    def _():
        kv_copy(1, at_chip(1), c_me, relay_send.at[0], kv_recv.at[1, 1]).wait_recv()
        kv_copy(1, at_chip(1), at_chip(3), relay_send.at[0], kv_recv.at[1, 1]).start()

    @pl.when(core == 1)
    def _():
        for h in range(kv_heads):
            sib_wait(chip, h)
            attend(sibling * rows, rows, h)

    def source(t):
        return lax.rem(chip - 1 + chip // 3 - t + 3, 3)

    relays = ((1, 0, 2, 0), (3, 0, 2, 1), (2, 1, 3, 0))

    def relay(a, frm, b, h):
        return kv_copy(h, at_chip(frm), at_chip(b), relay_send.at[0], kv_recv.at[frm, h])

    def take(t, h):
        src = source(t)
        kv_copy(h, at_chip(src), c_me, own_send.at[0, h], kv_recv.at[src, h]).wait_recv()
        for a, frm, b, hh in relays:
            if t == 0 and h == hh:
                @pl.when(chip == a)
                def _(a=a, frm=frm, b=b):
                    relay(a, frm, b, h).start()
        kv_copy(h, at_chip(src), sibling, fwd_send.at[src, h], fwd_recv.at[src, h]).start()

    def use_block(t, h):
        src = source(t)
        sib_wait(src, h)
        attend(src * 2 * rows, 2 * rows, h)

    @pl.when(chip == 3)
    def _():
        take(0, 1)
        take(1, 1)
        use_block(0, 1)
        take(0, 0)
        take(1, 0)
        use_block(1, 1)
        use_block(0, 0)
        take(2, 0)
        take(2, 1)
        use_block(1, 0)
        use_block(2, 0)
        use_block(2, 1)

    @pl.when((chip == 1) | (chip == 2))
    def _():
        take(0, 0)
        take(0, 1)
        use_block(0, 0)

    @pl.when(chip == 1)
    def _():
        use_block(0, 1)

    @pl.when(chip == 2)
    def _():
        use_block(0, 1)
        take(1, 1)
        take(1, 0)
        use_block(1, 1)
        use_block(1, 0)

    def finish_head(hd, carry):
        total = jnp.sum(l_v[hd], axis=1, keepdims=True)
        o_v[:, pl.ds(pl.multiple_of(hd * HEAD, HEAD), HEAD)] = (acc_v[hd] / total).astype(BF16)
        return carry
    lax.fori_loop(0, heads, finish_head, 0)

    wo_copy.wait()
    targets = (y_next, y_prev)
    dir_rows = (pl.ds(0, half), pl.ds(half, half))
    subs = (pl.ds(0, sub), pl.ds(sub, sub))

    def rs_copy(dr, s, u):
        return pltpu.make_async_remote_copy(
            src_ref=sbuf.at[dr, s, :, subs[u]], dst_ref=rbuf.at[dr, s, :, subs[u]],
            send_sem=rs_send.at[dr, s, u], recv_sem=rs_recv.at[dr, s, u],
            device_id={'tp': targets[dr]}, device_id_type=MESH)

    def ag_copy(dr, a, u, idx):
        ref = out_v.at[dir_rows[dr], pl.ds(pl.multiple_of(idx * chunk + u * sub, HEAD), sub)]
        return pltpu.make_async_remote_copy(
            src_ref=ref, dst_ref=ref, send_sem=ag_send.at[dr, a, u], recv_sem=ag_recv.at[dr, a, u],
            device_id={'tp': targets[dr]}, device_id_type=MESH)

    order = (y_prev, y_next, lax.rem(ty + 2, tp_n), ty)
    def project(i, r):
        cols = pl.ds(pl.multiple_of(order[i] * chunk, HEAD), chunk)
        return jnp.dot(o_v[r, :], wo_v[:, cols], preferred_element_type=F32)

    for dr in range(2):
        sbuf[dr, 0] = project(dr, dir_rows[dr]).astype(BF16)
        for u in range(2):
            rs_copy(dr, 0, u).start()
    for i in (2, 0, 1, 3):
        r = pl.ds(0, rows) if i > 1 else dir_rows[1 - i]
        part_v[i, r, :] = project(i, r)

    k_out[...] = jnp.stack([kv_v[i, 0, own_rows, :] for i in range(kv_heads)], axis=1)
    v_out[...] = jnp.stack([kv_v[i, 1, own_rows, :] for i in range(kv_heads)], axis=1)

    use = ((2, 1), (2, 0))
    for s in (1, 2):
        for u in range(2):
            for dr in range(2):
                rs_copy(dr, s - 1, u).wait_recv()
                got = rbuf[dr, s - 1, :, subs[u]].astype(F32)
                sbuf[dr, s, :, subs[u]] = (got + part_v[use[dr][s - 1], dir_rows[dr], subs[u]]).astype(BF16)
                rs_copy(dr, s, u).start()

    for u in range(2):
        for dr in range(2):
            rs_copy(dr, 2, u).wait_recv()
            cols = pl.ds(pl.multiple_of(ty * chunk + u * sub, HEAD), sub)
            a_sum = rbuf[dr, 2, :, subs[u]].astype(F32) + part_v[3, dir_rows[dr], subs[u]]
            out_v[dir_rows[dr], cols] = (x_v[dir_rows[dr], cols].astype(F32) + a_sum).astype(BF16)
            ag_copy(dr, 0, u, ty).start()

    def held(dr, a):
        return lax.rem(ty + tp_n - a, tp_n) if dr == 0 else lax.rem(ty + a, tp_n)

    for a in range(1, tp_n):
        for u in range(2):
            for dr in range(2):
                idx = held(dr, a)
                ag_copy(dr, a - 1, u, idx).wait_recv()
                if a < tp_n - 1:
                    ag_copy(dr, a, u, idx).start()

    for a in range(tp_n - 1):
        for u in range(2):
            for dr in range(2):
                rs_copy(dr, a, u).wait_send()
                ag_copy(dr, a, u, held(dr, a)).wait_send()
    for frm in range(chips):
        @pl.when(chip == frm)
        def _(frm=frm):
            for a, to, h, slot in plan:
                if a == frm:
                    own_copy(to, h, slot).wait_send()

    @pl.when(core == 0)
    def _():
        for h in range(kv_heads):
            sib_copy(h).wait_send()

    @pl.when(chip == 0)
    def _():
        kv_copy(1, at_chip(1), at_chip(3), relay_send.at[0], kv_recv.at[1, 1]).wait_send()

    for a, frm, b, h in relays:
        @pl.when(chip == a)
        def _(a=a, frm=frm, b=b, h=h):
            relay(a, frm, b, h).wait_send()
    for t in range(chips - 1):
        @pl.when(t < chip)
        def _(t=t):
            for h in range(kv_heads):
                kv_copy(h, at_chip(t), sibling, fwd_send.at[t, h], fwd_recv.at[t, h]).wait_send()


def store_kernel(out_v, k_v, v_v, out_hbm, k_hbm, v_hbm, sem):
    pairs = ((k_v, k_hbm), (v_v, v_hbm), (out_v, out_hbm))
    copies = [pltpu.make_async_copy(src, dst, sem.at[i]) for i, (src, dst) in enumerate(pairs)]
    for cp in copies:
        cp.start()
    for cp in copies:
        cp.wait()


def solution(mesh):
    tp_n = mesh.shape['tp']
    cp_n = mesh.shape['cp']
    row_spec = P(('dp', 'cp'), None)
    cache_spec = P(('dp', 'cp'), 'tp', None)
    head_cols = P(None, 'tp')

    def local_block(hidden, positions, norm_gain, w_query, w_key, w_value, w_out):
        rows, width = hidden.shape
        q_cols = w_query.shape[1]
        kv_cols = w_key.shape[1]
        heads = q_cols // HEAD
        kv_heads = kv_cols // HEAD
        chunk = width // tp_n
        half = rows // 2
        any_spec = pl.BlockSpec(memory_space=pl.ANY)
        vmem_spec = pl.BlockSpec(memory_space=pltpu.VMEM)
        dma = pltpu.SemaphoreType.DMA
        chips = cp_n // 2
        out, k_cache, v_cache = pl.pallas_call(
            functools.partial(block_kernel, tp_n, cp_n),
            out_shape=(pltpu.VMEM((rows, width), BF16),
                       pltpu.VMEM((rows, kv_heads, HEAD), BF16),
                       pltpu.VMEM((rows, kv_heads, HEAD), BF16)),
            in_specs=[any_spec, vmem_spec, vmem_spec, any_spec, any_spec, any_spec, any_spec],
            out_specs=(vmem_spec, vmem_spec, vmem_spec),
            scratch_shapes=[
                pltpu.VMEM((rows, width), BF16),
                pltpu.VMEM((rows, width), BF16),
                pltpu.VMEM((width, 2 * kv_cols), BF16),
                pltpu.VMEM((width, q_cols), BF16),
                pltpu.VMEM((q_cols, width), BF16),
                pltpu.VMEM((1, width), F32),
                pltpu.VMEM((rows, HEAD), F32),
                pltpu.VMEM((rows, HEAD), F32),
                pltpu.VMEM((heads, rows, HEAD), BF16),
                pltpu.VMEM((kv_heads, 2, cp_n * rows, HEAD), BF16),
                pltpu.VMEM((heads, rows, HEAD), F32),
                pltpu.VMEM((heads, rows, HEAD), F32),
                pltpu.VMEM((heads, rows, HEAD), F32),
                pltpu.VMEM((rows, q_cols), BF16),
                pltpu.VMEM((tp_n, rows, chunk), F32),
                pltpu.VMEM((2, tp_n - 1, half, chunk), BF16),
                pltpu.VMEM((2, tp_n - 1, half, chunk), BF16),
                pltpu.VMEM((rows, 2 * kv_cols), F32),
                dma((X_STRIPS,)), dma((2, KV_STRIPS)), dma((Q_STRIPS,)), dma,
                dma((2, kv_heads)), dma((1,)), dma((chips, kv_heads)), dma((chips, kv_heads)), dma((chips, kv_heads)),
                dma((2, tp_n - 1, 2)), dma((2, tp_n - 1, 2)), dma((2, tp_n - 1, 2)), dma((2, tp_n - 1, 2)),
            ],
            compiler_params=pltpu.CompilerParams(collective_id=0, has_side_effects=True, vmem_limit_bytes=VMEM_LIMIT),
        )(hidden, positions.reshape(1, rows), norm_gain.reshape(width // HEAD, HEAD), w_query, w_key, w_value, w_out)
        results = (out, k_cache, v_cache)
        return pl.pallas_call(
            store_kernel,
            out_shape=tuple(jax.ShapeDtypeStruct(r.shape, BF16) for r in results),
            in_specs=[vmem_spec] * 3,
            out_specs=(any_spec,) * 3,
            scratch_shapes=[dma((3,))],
        )(*[pltpu.with_memory_space_constraint(r, pltpu.VMEM) for r in results])

    return jax.shard_map(local_block, mesh=mesh, in_specs=(row_spec, P(('dp', 'cp')), P(None), head_cols, head_cols, head_cols, P('tp', None)), out_specs=(row_spec, cache_spec, cache_spec), check_vma=False)
```

```python
import math
import functools
import jax
import jax.numpy as jnp
from jax import lax
from jax.experimental import pallas as pl
from jax.experimental.pallas import tpu as pltpu
from jax.sharding import PartitionSpec as P

HEAD = 128
EPS = 1e-5
LOG_THETA = math.log(1000000.0)
EXP2_SCALE = math.log2(math.e) / math.sqrt(HEAD)
MESH = pl.DeviceIdType.MESH
F32 = jnp.float32
BF16 = jnp.bfloat16
MERGE = 4
X_STRIPS = 4
KV_STRIPS = 2
Q_STRIPS = 2
NORM_ROWS = 64
VMEM_LIMIT = 56 * 1024 * 1024


def block_kernel(tp_n, cp_n, x_hbm, pos_ref, gain_ref, wq_hbm, wk_hbm, wv_hbm, wo_hbm,
                 out_v, k_out, v_out,
                 x_v, h_v, wkv_v, wq_v, wo_v, gain_v, cos_v, sin_v, q_v, kv_v, m_v, l_v, acc_v, o_v,
                 part_v, sbuf, rbuf, kv_acc,
                 x_sem, wkv_sem, wq_sem, wo_sem,
                 own_send, relay_send, fwd_send, kv_recv, fwd_recv,
                 rs_send, rs_recv, ag_send, ag_recv):
    rows, width = x_v.shape
    chips = cp_n // 2
    heads = q_v.shape[0]
    kv_heads = kv_v.shape[0]
    group = heads // kv_heads
    half = rows // 2
    chunk = width // tp_n
    cut = chunk * 2 // 5
    ty = lax.axis_index('tp')
    c_me = lax.axis_index('cp')
    chip = c_me // 2
    core = lax.rem(c_me, 2)
    sibling = chip * 2 + (1 - core)

    strip = rows // X_STRIPS
    depth = width // KV_STRIPS
    kvw = kv_heads * HEAD
    qw = wq_v.shape[1] // Q_STRIPS
    x_copies = [pltpu.make_async_copy(x_hbm.at[pl.ds(i * strip, strip)], x_v.at[pl.ds(i * strip, strip)], x_sem.at[i])
                for i in range(X_STRIPS)]
    wkv_copies = [[pltpu.make_async_copy(w_hbm.at[pl.ds(i * depth, depth)],
                                         wkv_v.at[pl.ds(i * depth, depth), pl.ds(n * kvw, kvw)], wkv_sem.at[n, i])
                   for n, w_hbm in enumerate((wk_hbm, wv_hbm))] for i in range(KV_STRIPS)]
    wq_copies = [pltpu.make_async_copy(wq_hbm.at[:, pl.ds(j * qw, qw)], wq_v.at[:, pl.ds(j * qw, qw)], wq_sem.at[j])
                 for j in range(Q_STRIPS)]
    wo_copy = pltpu.make_async_copy(wo_hbm, wo_v, wo_sem)
    for cp in x_copies:
        cp.start()
    for pair in wkv_copies[:1]:
        for cp in pair:
            cp.start()

    barrier = pltpu.get_barrier_semaphore()
    y_next = lax.rem(ty + 1, tp_n)
    y_prev = lax.rem(ty + tp_n - 1, tp_n)
    partners = [{'tp': y_next}, {'tp': y_prev}, {'cp': sibling}]
    for d in range(1, chips):
        partners.append({'cp': lax.rem(c_me + 2 * d, cp_n)})
    for dev in partners:
        pl.semaphore_signal(barrier, inc=1, device_id=dev, device_id_type=MESH)

    freq = jnp.exp(lax.broadcasted_iota(jnp.int32, (HEAD // 2, rows), 0).astype(F32) * (-2.0 * LOG_THETA / HEAD))
    angles = pos_ref[...].astype(F32) * freq
    cos_t = jnp.cos(angles)
    sin_t = jnp.sin(angles)
    cos_v[...] = jnp.concatenate([cos_t, cos_t], axis=0).T
    sin_v[...] = jnp.concatenate([-sin_t, sin_t], axis=0).T

    gain_f = gain_ref[...].astype(F32)
    for i in range(width // HEAD):
        gain_v[:, i * HEAD:(i + 1) * HEAD] = gain_f[i:i + 1, :]

    for i in range(X_STRIPS):
        x_copies[i].wait()

        def norm_rows(n, carry, i=i):
            r = pl.ds(pl.multiple_of(i * strip + n * NORM_ROWS, NORM_ROWS), NORM_ROWS)
            xf = x_v[r, :].astype(F32)
            inv = lax.rsqrt(jnp.mean(xf * xf, axis=-1, keepdims=True) + EPS)
            h_v[r, :] = (xf * inv * gain_v[...]).astype(BF16)
            return carry
        lax.fori_loop(0, strip // NORM_ROWS, norm_rows, 0)
        if i == 0:
            for pair in wkv_copies[1:]:
                for cp in pair:
                    cp.start()
        if i == X_STRIPS - 1:
            for cp in wq_copies:
                cp.start()

    def rope(t):
        return t * cos_v[...] + pltpu.roll(t, HEAD // 2, 1) * sin_v[...]

    for i in range(KV_STRIPS):
        for cp in wkv_copies[i]:
            cp.wait()
        part_kv = jnp.dot(h_v[:, i * depth:(i + 1) * depth], wkv_v[i * depth:(i + 1) * depth, :], preferred_element_type=F32)
        if i == 0:
            kv_acc[...] = part_kv
        else:
            kv_acc[...] += part_kv
    kv_f = kv_acc[...]

    def kv_rows(c):
        return pl.ds(pl.multiple_of(c * rows, rows), rows)

    own_rows = kv_rows(c_me)
    for i in range(kv_heads):
        k_h = rope(kv_f[:, i * HEAD:(i + 1) * HEAD]).astype(BF16)
        kv_v[i, 0, own_rows, :] = k_h
        v_h = kv_f[:, kvw + i * HEAD:kvw + (i + 1) * HEAD].astype(BF16)
        kv_v[i, 1, own_rows, :] = v_h

    pl.semaphore_wait(barrier, len(partners))

    def kv_copy(h, src_c, target_c, ssem, rsem):
        ref = kv_v.at[h, :, kv_rows(src_c), :]
        return pltpu.make_async_remote_copy(src_ref=ref, dst_ref=ref, send_sem=ssem, recv_sem=rsem,
                                            device_id={'cp': target_c}, device_id_type=MESH)

    def at_chip(i):
        return i * 2 + core

    plan = ((0, 3, 1, 0), (0, 1, 0, 1), (0, 3, 0, 0), (0, 1, 1, 1), (1, 0, 1, 0), (1, 2, 0, 1), (1, 2, 1, 1), (2, 3, 1, 1), (2, 3, 0, 1))

    def own_copy(to, h, slot):
        return kv_copy(h, c_me, at_chip(to), own_send.at[slot, h], kv_recv.at[chip, h])

    def sib_copy(h):
        return kv_copy(h, c_me, sibling, fwd_send.at[chip, h], fwd_recv.at[chip, h])

    for frm in range(chips):
        @pl.when(chip == frm)
        def _(frm=frm):
            for a, to, h, slot in plan:
                if a == frm:
                    own_copy(to, h, slot).start()

    @pl.when(core == 0)
    def _():
        for h in range(kv_heads):
            sib_copy(h).start()

    for j in range(Q_STRIPS):
        wq_copies[j].wait()
        if j == Q_STRIPS - 1:
            wo_copy.start()
        q_f = jnp.dot(h_v[...], wq_v[:, j * qw:(j + 1) * qw], preferred_element_type=F32)
        for i in range(qw // HEAD):
            q_v[j * (qw // HEAD) + i] = rope(q_f[:, i * HEAD:(i + 1) * HEAD]).astype(BF16)

    span = MERGE * rows

    def merged(ref, hd):
        return ref[pl.ds(hd, MERGE)].reshape(span, HEAD)

    def put(ref, hd, val):
        ref[pl.ds(hd, MERGE)] = val.reshape(MERGE, rows, HEAD)

    def tiles(s):
        return [s[:, i * HEAD:(i + 1) * HEAD] for i in range(s.shape[1] // HEAD)]

    def scores(hd, kh, keys):
        return lax.dot_general(merged(q_v, hd), kv_v[kh, 0, keys, :], (((1,), (1,)), ((), ())), preferred_element_type=F32)

    def row_max(s):
        return jnp.broadcast_to(jnp.max(functools.reduce(jnp.maximum, tiles(s)), axis=1, keepdims=True), (span, HEAD))

    def own_heads(i, carry):
        hd = i * MERGE
        kh = hd // group
        s = scores(hd, kh, own_rows)
        r_i = lax.rem(lax.broadcasted_iota(jnp.int32, (span, rows), 0), rows)
        c_i = lax.broadcasted_iota(jnp.int32, (span, rows), 1)
        s = jnp.where(c_i <= r_i, s, -jnp.inf)
        m = row_max(s)
        ps = [jnp.exp2((t - m) * EXP2_SCALE) for t in tiles(s)]
        p = jnp.concatenate([t.astype(BF16) for t in ps], axis=1)
        put(m_v, hd, m)
        put(l_v, hd, functools.reduce(jnp.add, ps))
        put(acc_v, hd, jnp.dot(p, kv_v[kh, 1, own_rows, :], preferred_element_type=F32))
        return carry
    lax.fori_loop(0, heads // MERGE, own_heads, 0)

    def attend(start, count, kh):
        keys = pl.ds(pl.multiple_of(start, rows), count)

        def some_heads(i, carry):
            hd = kh * group + i * MERGE
            s = scores(hd, kh, keys)
            old = merged(m_v, hd)
            new = jnp.maximum(old, row_max(s))
            alpha = jnp.exp2((old - new) * EXP2_SCALE)
            ps = [jnp.exp2((t - new) * EXP2_SCALE) for t in tiles(s)]
            p = jnp.concatenate([t.astype(BF16) for t in ps], axis=1)
            put(m_v, hd, new)
            put(l_v, hd, merged(l_v, hd) * alpha + functools.reduce(jnp.add, ps))
            put(acc_v, hd, merged(acc_v, hd) * alpha + jnp.dot(p, kv_v[kh, 1, keys, :], preferred_element_type=F32))
            return carry
        lax.fori_loop(0, group // MERGE, some_heads, 0)

    def sib_wait(i, h):
        kv_copy(h, 2 * i + 1 - core, c_me, fwd_send.at[i, h], fwd_recv.at[i, h]).wait_recv()

    @pl.when(chip == 0)
    def _():
        kv_copy(1, at_chip(1), c_me, relay_send.at[0], kv_recv.at[1, 1]).wait_recv()
        kv_copy(1, at_chip(1), at_chip(3), relay_send.at[0], kv_recv.at[1, 1]).start()

    @pl.when(core == 1)
    def _():
        for h in range(kv_heads):
            sib_wait(chip, h)
            attend(sibling * rows, rows, h)

    def source(t):
        return lax.rem(chip - 1 + chip // 3 - t + 3, 3)

    relays = ((1, 0, 2, 0), (3, 0, 2, 1), (2, 1, 3, 0))

    def relay(a, frm, b, h):
        return kv_copy(h, at_chip(frm), at_chip(b), relay_send.at[0], kv_recv.at[frm, h])

    def take(t, h):
        src = source(t)
        kv_copy(h, at_chip(src), c_me, own_send.at[0, h], kv_recv.at[src, h]).wait_recv()
        for a, frm, b, hh in relays:
            if t == 0 and h == hh:
                @pl.when(chip == a)
                def _(a=a, frm=frm, b=b):
                    relay(a, frm, b, h).start()
        kv_copy(h, at_chip(src), sibling, fwd_send.at[src, h], fwd_recv.at[src, h]).start()

    def use_direct(t, h):
        attend((source(t) * 2 + core) * rows, rows, h)

    def use_passed(t, h):
        src = source(t)
        sib_wait(src, h)
        attend((src * 2 + 1 - core) * rows, rows, h)

    def use_block(t, h):
        src = source(t)
        sib_wait(src, h)
        attend(src * 2 * rows, 2 * rows, h)

    @pl.when(chip == 3)
    def _():
        take(0, 1)
        take(1, 1)
        use_direct(0, 1)
        use_direct(1, 1)
        use_passed(0, 1)
        take(0, 0)
        take(1, 0)
        use_passed(1, 1)
        use_block(0, 0)
        take(2, 0)
        take(2, 1)
        use_block(1, 0)
        use_block(2, 0)
        use_block(2, 1)

    @pl.when((chip == 1) | (chip == 2))
    def _():
        take(0, 0)
        take(0, 1)
        use_block(0, 0)

    @pl.when(chip == 1)
    def _():
        use_block(0, 1)

    @pl.when(chip == 2)
    def _():
        use_block(0, 1)
        take(1, 1)
        take(1, 0)
        use_direct(1, 1)
        use_direct(1, 0)
        use_passed(1, 1)
        use_passed(1, 0)

    def finish_head(hd, carry):
        total = jnp.sum(l_v[hd], axis=1, keepdims=True)
        o_v[:, pl.ds(pl.multiple_of(hd * HEAD, HEAD), HEAD)] = (acc_v[hd] / total).astype(BF16)
        return carry
    lax.fori_loop(0, heads, finish_head, 0)

    wo_copy.wait()
    targets = (y_next, y_prev)
    dir_rows = (pl.ds(0, half), pl.ds(half, half))
    subs = (pl.ds(0, cut), pl.ds(cut, chunk - cut))
    starts = (0, cut)
    sizes = (cut, chunk - cut)

    def rs_copy(dr, s, u):
        return pltpu.make_async_remote_copy(
            src_ref=sbuf.at[dr, s, :, subs[u]], dst_ref=rbuf.at[dr, s, :, subs[u]],
            send_sem=rs_send.at[dr, s, u], recv_sem=rs_recv.at[dr, s, u],
            device_id={'tp': targets[dr]}, device_id_type=MESH)

    def ag_copy(dr, a, u, idx):
        ref = out_v.at[dir_rows[dr], pl.ds(pl.multiple_of(idx * chunk + starts[u], HEAD), sizes[u])]
        return pltpu.make_async_remote_copy(
            src_ref=ref, dst_ref=ref, send_sem=ag_send.at[dr, a, u], recv_sem=ag_recv.at[dr, a, u],
            device_id={'tp': targets[dr]}, device_id_type=MESH)

    order = (y_prev, y_next, lax.rem(ty + 2, tp_n), ty)
    def project(i, r, first=0, size=chunk):
        cols = pl.ds(pl.multiple_of(order[i] * chunk + first, HEAD), size)
        return jnp.dot(o_v[r, :], wo_v[:, cols], preferred_element_type=F32)

    for u in range(2):
        for dr in range(2):
            sbuf[dr, 0, :, subs[u]] = project(dr, dir_rows[dr], starts[u], sizes[u]).astype(BF16)
            rs_copy(dr, 0, u).start()
    for i in (2, 0, 1, 3):
        r = pl.ds(0, rows) if i > 1 else dir_rows[1 - i]
        part_v[i, r, :] = project(i, r)

    k_out[...] = jnp.stack([kv_v[i, 0, own_rows, :] for i in range(kv_heads)], axis=1)
    v_out[...] = jnp.stack([kv_v[i, 1, own_rows, :] for i in range(kv_heads)], axis=1)

    use = ((2, 1), (2, 0))
    for s in (1, 2):
        for u in range(2):
            for dr in range(2):
                rs_copy(dr, s - 1, u).wait_recv()
                got = rbuf[dr, s - 1, :, subs[u]].astype(F32)
                sbuf[dr, s, :, subs[u]] = (got + part_v[use[dr][s - 1], dir_rows[dr], subs[u]]).astype(BF16)
                rs_copy(dr, s, u).start()

    for u in range(2):
        for dr in range(2):
            rs_copy(dr, 2, u).wait_recv()
            cols = pl.ds(pl.multiple_of(ty * chunk + starts[u], HEAD), sizes[u])
            a_sum = rbuf[dr, 2, :, subs[u]].astype(F32) + part_v[3, dir_rows[dr], subs[u]]
            out_v[dir_rows[dr], cols] = (x_v[dir_rows[dr], cols].astype(F32) + a_sum).astype(BF16)
            ag_copy(dr, 0, u, ty).start()

    def held(dr, a):
        return lax.rem(ty + tp_n - a, tp_n) if dr == 0 else lax.rem(ty + a, tp_n)

    for a in range(1, tp_n):
        for u in range(2):
            for dr in range(2):
                idx = held(dr, a)
                ag_copy(dr, a - 1, u, idx).wait_recv()
                if a < tp_n - 1:
                    ag_copy(dr, a, u, idx).start()

    for a in range(tp_n - 1):
        for u in range(2):
            for dr in range(2):
                rs_copy(dr, a, u).wait_send()
                ag_copy(dr, a, u, held(dr, a)).wait_send()
    for frm in range(chips):
        @pl.when(chip == frm)
        def _(frm=frm):
            for a, to, h, slot in plan:
                if a == frm:
                    own_copy(to, h, slot).wait_send()

    @pl.when(core == 0)
    def _():
        for h in range(kv_heads):
            sib_copy(h).wait_send()

    @pl.when(chip == 0)
    def _():
        kv_copy(1, at_chip(1), at_chip(3), relay_send.at[0], kv_recv.at[1, 1]).wait_send()

    for a, frm, b, h in relays:
        @pl.when(chip == a)
        def _(a=a, frm=frm, b=b, h=h):
            relay(a, frm, b, h).wait_send()
    for t in range(chips - 1):
        @pl.when(t < chip)
        def _(t=t):
            for h in range(kv_heads):
                kv_copy(h, at_chip(t), sibling, fwd_send.at[t, h], fwd_recv.at[t, h]).wait_send()


def store_kernel(out_v, k_v, v_v, out_hbm, k_hbm, v_hbm, sem):
    pairs = ((k_v, k_hbm), (v_v, v_hbm), (out_v, out_hbm))
    copies = [pltpu.make_async_copy(src, dst, sem.at[i]) for i, (src, dst) in enumerate(pairs)]
    for cp in copies:
        cp.start()
    for cp in copies:
        cp.wait()


def solution(mesh):
    tp_n = mesh.shape['tp']
    cp_n = mesh.shape['cp']
    row_spec = P(('dp', 'cp'), None)
    cache_spec = P(('dp', 'cp'), 'tp', None)
    head_cols = P(None, 'tp')

    def local_block(hidden, positions, norm_gain, w_query, w_key, w_value, w_out):
        rows, width = hidden.shape
        q_cols = w_query.shape[1]
        kv_cols = w_key.shape[1]
        heads = q_cols // HEAD
        kv_heads = kv_cols // HEAD
        chunk = width // tp_n
        half = rows // 2
        any_spec = pl.BlockSpec(memory_space=pl.ANY)
        vmem_spec = pl.BlockSpec(memory_space=pltpu.VMEM)
        dma = pltpu.SemaphoreType.DMA
        chips = cp_n // 2
        out, k_cache, v_cache = pl.pallas_call(
            functools.partial(block_kernel, tp_n, cp_n),
            out_shape=(pltpu.VMEM((rows, width), BF16),
                       pltpu.VMEM((rows, kv_heads, HEAD), BF16),
                       pltpu.VMEM((rows, kv_heads, HEAD), BF16)),
            in_specs=[any_spec, vmem_spec, vmem_spec, any_spec, any_spec, any_spec, any_spec],
            out_specs=(vmem_spec, vmem_spec, vmem_spec),
            scratch_shapes=[
                pltpu.VMEM((rows, width), BF16),
                pltpu.VMEM((rows, width), BF16),
                pltpu.VMEM((width, 2 * kv_cols), BF16),
                pltpu.VMEM((width, q_cols), BF16),
                pltpu.VMEM((q_cols, width), BF16),
                pltpu.VMEM((1, width), F32),
                pltpu.VMEM((rows, HEAD), F32),
                pltpu.VMEM((rows, HEAD), F32),
                pltpu.VMEM((heads, rows, HEAD), BF16),
                pltpu.VMEM((kv_heads, 2, cp_n * rows, HEAD), BF16),
                pltpu.VMEM((heads, rows, HEAD), F32),
                pltpu.VMEM((heads, rows, HEAD), F32),
                pltpu.VMEM((heads, rows, HEAD), F32),
                pltpu.VMEM((rows, q_cols), BF16),
                pltpu.VMEM((tp_n, rows, chunk), F32),
                pltpu.VMEM((2, tp_n - 1, half, chunk), BF16),
                pltpu.VMEM((2, tp_n - 1, half, chunk), BF16),
                pltpu.VMEM((rows, 2 * kv_cols), F32),
                dma((X_STRIPS,)), dma((2, KV_STRIPS)), dma((Q_STRIPS,)), dma,
                dma((2, kv_heads)), dma((1,)), dma((chips, kv_heads)), dma((chips, kv_heads)), dma((chips, kv_heads)),
                dma((2, tp_n - 1, 2)), dma((2, tp_n - 1, 2)), dma((2, tp_n - 1, 2)), dma((2, tp_n - 1, 2)),
            ],
            compiler_params=pltpu.CompilerParams(collective_id=0, has_side_effects=True, vmem_limit_bytes=VMEM_LIMIT),
        )(hidden, positions.reshape(1, rows), norm_gain.reshape(width // HEAD, HEAD), w_query, w_key, w_value, w_out)
        results = (out, k_cache, v_cache)
        return pl.pallas_call(
            store_kernel,
            out_shape=tuple(jax.ShapeDtypeStruct(r.shape, BF16) for r in results),
            in_specs=[vmem_spec] * 3,
            out_specs=(any_spec,) * 3,
            scratch_shapes=[dma((3,))],
        )(*[pltpu.with_memory_space_constraint(r, pltpu.VMEM) for r in results])

    return jax.shard_map(local_block, mesh=mesh, in_specs=(row_spec, P(('dp', 'cp')), P(None), head_cols, head_cols, head_cols, P('tp', None)), out_specs=(row_spec, cache_spec, cache_spec), check_vma=False)
```

```python
import math
import functools
import jax
import jax.numpy as jnp
from jax import lax
from jax.experimental import pallas as pl
from jax.experimental.pallas import tpu as pltpu
from jax.sharding import PartitionSpec as P

HEAD = 128
EPS = 1e-5
LOG_THETA = math.log(1000000.0)
EXP2_SCALE = math.log2(math.e) / math.sqrt(HEAD)
MESH = pl.DeviceIdType.MESH
F32 = jnp.float32
BF16 = jnp.bfloat16
MERGE = 4
X_STRIPS = 4
KV_STRIPS = 2
Q_STRIPS = 2
NORM_ROWS = 64
VMEM_LIMIT = 56 * 1024 * 1024


def block_kernel(tp_n, cp_n, x_hbm, pos_ref, gain_ref, wq_hbm, wk_hbm, wv_hbm, wo_hbm,
                 out_v, k_out, v_out,
                 x_v, h_v, wkv_v, wq_v, wo_v, gain_v, cos_v, sin_v, q_v, kv_v, m_v, l_v, acc_v, o_v,
                 part_v, sbuf, rbuf, kv_acc,
                 x_sem, wkv_sem, wq_sem, wo_sem,
                 own_send, relay_send, fwd_send, kv_recv, fwd_recv,
                 rs_send, rs_recv, ag_send, ag_recv):
    rows, width = x_v.shape
    chips = cp_n // 2
    heads = q_v.shape[0]
    kv_heads = kv_v.shape[0]
    group = heads // kv_heads
    half = rows // 2
    chunk = width // tp_n
    cut = chunk * 2 // 5
    ty = lax.axis_index('tp')
    c_me = lax.axis_index('cp')
    chip = c_me // 2
    core = lax.rem(c_me, 2)
    sibling = chip * 2 + (1 - core)

    strip = rows // X_STRIPS
    depth = width // KV_STRIPS
    kvw = kv_heads * HEAD
    qw = wq_v.shape[1] // Q_STRIPS
    x_copies = [pltpu.make_async_copy(x_hbm.at[pl.ds(i * strip, strip)], x_v.at[pl.ds(i * strip, strip)], x_sem.at[i])
                for i in range(X_STRIPS)]
    wkv_copies = [[pltpu.make_async_copy(w_hbm.at[pl.ds(i * depth, depth)],
                                         wkv_v.at[pl.ds(i * depth, depth), pl.ds(n * kvw, kvw)], wkv_sem.at[n, i])
                   for n, w_hbm in enumerate((wk_hbm, wv_hbm))] for i in range(KV_STRIPS)]
    wq_copies = [pltpu.make_async_copy(wq_hbm.at[:, pl.ds(j * qw, qw)], wq_v.at[:, pl.ds(j * qw, qw)], wq_sem.at[j])
                 for j in range(Q_STRIPS)]
    wo_copy = pltpu.make_async_copy(wo_hbm, wo_v, wo_sem)
    for cp in x_copies:
        cp.start()
    for pair in wkv_copies[:1]:
        for cp in pair:
            cp.start()

    barrier = pltpu.get_barrier_semaphore()
    y_next = lax.rem(ty + 1, tp_n)
    y_prev = lax.rem(ty + tp_n - 1, tp_n)
    partners = [{'tp': y_next}, {'tp': y_prev}, {'cp': sibling}]
    for d in range(1, chips):
        partners.append({'cp': lax.rem(c_me + 2 * d, cp_n)})
    for dev in partners:
        pl.semaphore_signal(barrier, inc=1, device_id=dev, device_id_type=MESH)

    freq = jnp.exp(lax.broadcasted_iota(jnp.int32, (HEAD // 2, rows), 0).astype(F32) * (-2.0 * LOG_THETA / HEAD))
    angles = pos_ref[...].astype(F32) * freq
    cos_t = jnp.cos(angles)
    sin_t = jnp.sin(angles)
    cos_v[...] = jnp.concatenate([cos_t, cos_t], axis=0).T
    sin_v[...] = jnp.concatenate([-sin_t, sin_t], axis=0).T

    gain_f = gain_ref[...].astype(F32)
    for i in range(width // HEAD):
        gain_v[:, i * HEAD:(i + 1) * HEAD] = gain_f[i:i + 1, :]

    for i in range(X_STRIPS):
        x_copies[i].wait()

        def norm_rows(n, carry, i=i):
            r = pl.ds(pl.multiple_of(i * strip + n * NORM_ROWS, NORM_ROWS), NORM_ROWS)
            xf = x_v[r, :].astype(F32)
            inv = lax.rsqrt(jnp.mean(xf * xf, axis=-1, keepdims=True) + EPS)
            h_v[r, :] = (xf * inv * gain_v[...]).astype(BF16)
            return carry
        lax.fori_loop(0, strip // NORM_ROWS, norm_rows, 0)
        if i == 0:
            for pair in wkv_copies[1:]:
                for cp in pair:
                    cp.start()
        if i == X_STRIPS - 1:
            for cp in wq_copies:
                cp.start()

    def rope(t):
        return t * cos_v[...] + pltpu.roll(t, HEAD // 2, 1) * sin_v[...]

    for i in range(KV_STRIPS):
        for cp in wkv_copies[i]:
            cp.wait()
        part_kv = jnp.dot(h_v[:, i * depth:(i + 1) * depth], wkv_v[i * depth:(i + 1) * depth, :], preferred_element_type=F32)
        if i == 0:
            kv_acc[...] = part_kv
        else:
            kv_acc[...] += part_kv
    kv_f = kv_acc[...]

    def kv_rows(c):
        return pl.ds(pl.multiple_of(c * rows, rows), rows)

    own_rows = kv_rows(c_me)
    for i in range(kv_heads):
        k_h = rope(kv_f[:, i * HEAD:(i + 1) * HEAD]).astype(BF16)
        kv_v[i, 0, own_rows, :] = k_h
        v_h = kv_f[:, kvw + i * HEAD:kvw + (i + 1) * HEAD].astype(BF16)
        kv_v[i, 1, own_rows, :] = v_h

    pl.semaphore_wait(barrier, len(partners))

    def kv_copy(h, src_c, target_c, ssem, rsem):
        ref = kv_v.at[h, :, kv_rows(src_c), :]
        return pltpu.make_async_remote_copy(src_ref=ref, dst_ref=ref, send_sem=ssem, recv_sem=rsem,
                                            device_id={'cp': target_c}, device_id_type=MESH)

    def at_chip(i):
        return i * 2 + core

    plan = ((0, 3, 1, 0), (0, 1, 0, 1), (0, 3, 0, 0), (0, 1, 1, 1), (1, 0, 1, 0), (1, 2, 0, 1), (1, 2, 1, 1), (2, 3, 1, 1), (2, 3, 0, 1))

    def own_copy(to, h, slot):
        return kv_copy(h, c_me, at_chip(to), own_send.at[slot, h], kv_recv.at[chip, h])

    def sib_copy(h):
        return kv_copy(h, c_me, sibling, fwd_send.at[chip, h], fwd_recv.at[chip, h])

    for frm in range(chips):
        @pl.when(chip == frm)
        def _(frm=frm):
            for a, to, h, slot in plan:
                if a == frm:
                    own_copy(to, h, slot).start()

    @pl.when(core == 0)
    def _():
        for h in range(kv_heads):
            sib_copy(h).start()

    for j in range(Q_STRIPS):
        wq_copies[j].wait()
        if j == Q_STRIPS - 1:
            wo_copy.start()
        q_f = jnp.dot(h_v[...], wq_v[:, j * qw:(j + 1) * qw], preferred_element_type=F32)
        for i in range(qw // HEAD):
            q_v[j * (qw // HEAD) + i] = rope(q_f[:, i * HEAD:(i + 1) * HEAD]).astype(BF16)

    span = MERGE * rows

    def merged(ref, hd):
        return ref[pl.ds(hd, MERGE)].reshape(span, HEAD)

    def put(ref, hd, val):
        ref[pl.ds(hd, MERGE)] = val.reshape(MERGE, rows, HEAD)

    def tiles(s):
        return [s[:, i * HEAD:(i + 1) * HEAD] for i in range(s.shape[1] // HEAD)]

    def scores(hd, kh, keys):
        return lax.dot_general(merged(q_v, hd), kv_v[kh, 0, keys, :], (((1,), (1,)), ((), ())), preferred_element_type=F32)

    def row_max(s):
        return jnp.broadcast_to(jnp.max(functools.reduce(jnp.maximum, tiles(s)), axis=1, keepdims=True), (span, HEAD))

    def own_heads(i, carry):
        hd = i * MERGE
        kh = hd // group
        s = scores(hd, kh, own_rows)
        r_i = lax.rem(lax.broadcasted_iota(jnp.int32, (span, rows), 0), rows)
        c_i = lax.broadcasted_iota(jnp.int32, (span, rows), 1)
        s = jnp.where(c_i <= r_i, s, -jnp.inf)
        m = row_max(s)
        ps = [jnp.exp2((t - m) * EXP2_SCALE) for t in tiles(s)]
        p = jnp.concatenate([t.astype(BF16) for t in ps], axis=1)
        put(m_v, hd, m)
        put(l_v, hd, functools.reduce(jnp.add, ps))
        put(acc_v, hd, jnp.dot(p, kv_v[kh, 1, own_rows, :], preferred_element_type=F32))
        return carry
    lax.fori_loop(0, heads // MERGE, own_heads, 0, unroll=True)

    def attend(start, count, kh):
        keys = pl.ds(pl.multiple_of(start, rows), count)

        def some_heads(i, carry):
            hd = kh * group + i * MERGE
            s = scores(hd, kh, keys)
            old = merged(m_v, hd)
            new = jnp.maximum(old, row_max(s))
            alpha = jnp.exp2((old - new) * EXP2_SCALE)
            ps = [jnp.exp2((t - new) * EXP2_SCALE) for t in tiles(s)]
            p = jnp.concatenate([t.astype(BF16) for t in ps], axis=1)
            put(m_v, hd, new)
            put(l_v, hd, merged(l_v, hd) * alpha + functools.reduce(jnp.add, ps))
            put(acc_v, hd, merged(acc_v, hd) * alpha + jnp.dot(p, kv_v[kh, 1, keys, :], preferred_element_type=F32))
            return carry
        lax.fori_loop(0, group // MERGE, some_heads, 0)

    def sib_wait(i, h):
        kv_copy(h, 2 * i + 1 - core, c_me, fwd_send.at[i, h], fwd_recv.at[i, h]).wait_recv()

    @pl.when(chip == 0)
    def _():
        kv_copy(1, at_chip(1), c_me, relay_send.at[0], kv_recv.at[1, 1]).wait_recv()
        kv_copy(1, at_chip(1), at_chip(3), relay_send.at[0], kv_recv.at[1, 1]).start()

    @pl.when(core == 1)
    def _():
        for h in range(kv_heads):
            sib_wait(chip, h)
            attend(sibling * rows, rows, h)

    def source(t):
        return lax.rem(chip - 1 + chip // 3 - t + 3, 3)

    relays = ((1, 0, 2, 0), (3, 0, 2, 1), (2, 1, 3, 0))

    def relay(a, frm, b, h):
        return kv_copy(h, at_chip(frm), at_chip(b), relay_send.at[0], kv_recv.at[frm, h])

    def take(t, h):
        src = source(t)
        kv_copy(h, at_chip(src), c_me, own_send.at[0, h], kv_recv.at[src, h]).wait_recv()
        for a, frm, b, hh in relays:
            if t == 0 and h == hh:
                @pl.when(chip == a)
                def _(a=a, frm=frm, b=b):
                    relay(a, frm, b, h).start()
        kv_copy(h, at_chip(src), sibling, fwd_send.at[src, h], fwd_recv.at[src, h]).start()

    def use_direct(t, h):
        attend((source(t) * 2 + core) * rows, rows, h)

    def use_passed(t, h):
        src = source(t)
        sib_wait(src, h)
        attend((src * 2 + 1 - core) * rows, rows, h)

    def use_block(t, h):
        src = source(t)
        sib_wait(src, h)
        attend(src * 2 * rows, 2 * rows, h)

    @pl.when(chip == 3)
    def _():
        take(0, 1)
        take(1, 1)
        use_direct(0, 1)
        use_direct(1, 1)
        use_passed(0, 1)
        take(0, 0)
        take(1, 0)
        use_passed(1, 1)
        use_block(0, 0)
        take(2, 0)
        take(2, 1)
        use_block(1, 0)
        use_block(2, 0)
        use_block(2, 1)

    @pl.when((chip == 1) | (chip == 2))
    def _():
        take(0, 0)
        take(0, 1)
        use_block(0, 0)

    @pl.when(chip == 1)
    def _():
        use_block(0, 1)

    @pl.when(chip == 2)
    def _():
        use_block(0, 1)
        take(1, 1)
        take(1, 0)
        use_direct(1, 1)
        use_direct(1, 0)
        use_passed(1, 1)
        use_passed(1, 0)

    def finish_head(hd, carry):
        total = jnp.sum(l_v[hd], axis=1, keepdims=True)
        o_v[:, pl.ds(pl.multiple_of(hd * HEAD, HEAD), HEAD)] = (acc_v[hd] / total).astype(BF16)
        return carry
    lax.fori_loop(0, heads, finish_head, 0, unroll=True)

    wo_copy.wait()
    targets = (y_next, y_prev)
    dir_rows = (pl.ds(0, half), pl.ds(half, half))
    subs = (pl.ds(0, cut), pl.ds(cut, chunk - cut))
    starts = (0, cut)
    sizes = (cut, chunk - cut)

    def rs_copy(dr, s, u):
        return pltpu.make_async_remote_copy(
            src_ref=sbuf.at[dr, s, :, subs[u]], dst_ref=rbuf.at[dr, s, :, subs[u]],
            send_sem=rs_send.at[dr, s, u], recv_sem=rs_recv.at[dr, s, u],
            device_id={'tp': targets[dr]}, device_id_type=MESH)

    def ag_copy(dr, a, u, idx):
        ref = out_v.at[dir_rows[dr], pl.ds(pl.multiple_of(idx * chunk + starts[u], HEAD), sizes[u])]
        return pltpu.make_async_remote_copy(
            src_ref=ref, dst_ref=ref, send_sem=ag_send.at[dr, a, u], recv_sem=ag_recv.at[dr, a, u],
            device_id={'tp': targets[dr]}, device_id_type=MESH)

    order = (y_prev, y_next, lax.rem(ty + 2, tp_n), ty)
    def project(i, r, first=0, size=chunk):
        cols = pl.ds(pl.multiple_of(order[i] * chunk + first, HEAD), size)
        return jnp.dot(o_v[r, :], wo_v[:, cols], preferred_element_type=F32)

    for u in range(2):
        for dr in range(2):
            sbuf[dr, 0, :, subs[u]] = project(dr, dir_rows[dr], starts[u], sizes[u]).astype(BF16)
            rs_copy(dr, 0, u).start()
    for i in (2, 0, 1, 3):
        r = pl.ds(0, rows) if i > 1 else dir_rows[1 - i]
        part_v[i, r, :] = project(i, r)

    k_out[...] = jnp.stack([kv_v[i, 0, own_rows, :] for i in range(kv_heads)], axis=1)
    v_out[...] = jnp.stack([kv_v[i, 1, own_rows, :] for i in range(kv_heads)], axis=1)

    use = ((2, 1), (2, 0))
    for s in (1, 2):
        for u in range(2):
            for dr in range(2):
                rs_copy(dr, s - 1, u).wait_recv()
                got = rbuf[dr, s - 1, :, subs[u]].astype(F32)
                sbuf[dr, s, :, subs[u]] = (got + part_v[use[dr][s - 1], dir_rows[dr], subs[u]]).astype(BF16)
                rs_copy(dr, s, u).start()

    for u in range(2):
        for dr in range(2):
            rs_copy(dr, 2, u).wait_recv()
            cols = pl.ds(pl.multiple_of(ty * chunk + starts[u], HEAD), sizes[u])
            a_sum = rbuf[dr, 2, :, subs[u]].astype(F32) + part_v[3, dir_rows[dr], subs[u]]
            out_v[dir_rows[dr], cols] = (x_v[dir_rows[dr], cols].astype(F32) + a_sum).astype(BF16)
            ag_copy(dr, 0, u, ty).start()

    def held(dr, a):
        return lax.rem(ty + tp_n - a, tp_n) if dr == 0 else lax.rem(ty + a, tp_n)

    for a in range(1, tp_n):
        for u in range(2):
            for dr in range(2):
                idx = held(dr, a)
                ag_copy(dr, a - 1, u, idx).wait_recv()
                if a < tp_n - 1:
                    ag_copy(dr, a, u, idx).start()

    for a in range(tp_n - 1):
        for u in range(2):
            for dr in range(2):
                rs_copy(dr, a, u).wait_send()
                ag_copy(dr, a, u, held(dr, a)).wait_send()
    for frm in range(chips):
        @pl.when(chip == frm)
        def _(frm=frm):
            for a, to, h, slot in plan:
                if a == frm:
                    own_copy(to, h, slot).wait_send()

    @pl.when(core == 0)
    def _():
        for h in range(kv_heads):
            sib_copy(h).wait_send()

    @pl.when(chip == 0)
    def _():
        kv_copy(1, at_chip(1), at_chip(3), relay_send.at[0], kv_recv.at[1, 1]).wait_send()

    for a, frm, b, h in relays:
        @pl.when(chip == a)
        def _(a=a, frm=frm, b=b, h=h):
            relay(a, frm, b, h).wait_send()
    for t in range(chips - 1):
        @pl.when(t < chip)
        def _(t=t):
            for h in range(kv_heads):
                kv_copy(h, at_chip(t), sibling, fwd_send.at[t, h], fwd_recv.at[t, h]).wait_send()


def store_kernel(out_v, k_v, v_v, out_hbm, k_hbm, v_hbm, sem):
    pairs = ((k_v, k_hbm), (v_v, v_hbm), (out_v, out_hbm))
    copies = [pltpu.make_async_copy(src, dst, sem.at[i]) for i, (src, dst) in enumerate(pairs)]
    for cp in copies:
        cp.start()
    for cp in copies:
        cp.wait()


def solution(mesh):
    tp_n = mesh.shape['tp']
    cp_n = mesh.shape['cp']
    row_spec = P(('dp', 'cp'), None)
    cache_spec = P(('dp', 'cp'), 'tp', None)
    head_cols = P(None, 'tp')

    def local_block(hidden, positions, norm_gain, w_query, w_key, w_value, w_out):
        rows, width = hidden.shape
        q_cols = w_query.shape[1]
        kv_cols = w_key.shape[1]
        heads = q_cols // HEAD
        kv_heads = kv_cols // HEAD
        chunk = width // tp_n
        half = rows // 2
        any_spec = pl.BlockSpec(memory_space=pl.ANY)
        vmem_spec = pl.BlockSpec(memory_space=pltpu.VMEM)
        dma = pltpu.SemaphoreType.DMA
        chips = cp_n // 2
        out, k_cache, v_cache = pl.pallas_call(
            functools.partial(block_kernel, tp_n, cp_n),
            out_shape=(pltpu.VMEM((rows, width), BF16),
                       pltpu.VMEM((rows, kv_heads, HEAD), BF16),
                       pltpu.VMEM((rows, kv_heads, HEAD), BF16)),
            in_specs=[any_spec, vmem_spec, vmem_spec, any_spec, any_spec, any_spec, any_spec],
            out_specs=(vmem_spec, vmem_spec, vmem_spec),
            scratch_shapes=[
                pltpu.VMEM((rows, width), BF16),
                pltpu.VMEM((rows, width), BF16),
                pltpu.VMEM((width, 2 * kv_cols), BF16),
                pltpu.VMEM((width, q_cols), BF16),
                pltpu.VMEM((q_cols, width), BF16),
                pltpu.VMEM((1, width), F32),
                pltpu.VMEM((rows, HEAD), F32),
                pltpu.VMEM((rows, HEAD), F32),
                pltpu.VMEM((heads, rows, HEAD), BF16),
                pltpu.VMEM((kv_heads, 2, cp_n * rows, HEAD), BF16),
                pltpu.VMEM((heads, rows, HEAD), F32),
                pltpu.VMEM((heads, rows, HEAD), F32),
                pltpu.VMEM((heads, rows, HEAD), F32),
                pltpu.VMEM((rows, q_cols), BF16),
                pltpu.VMEM((tp_n, rows, chunk), F32),
                pltpu.VMEM((2, tp_n - 1, half, chunk), BF16),
                pltpu.VMEM((2, tp_n - 1, half, chunk), BF16),
                pltpu.VMEM((rows, 2 * kv_cols), F32),
                dma((X_STRIPS,)), dma((2, KV_STRIPS)), dma((Q_STRIPS,)), dma,
                dma((2, kv_heads)), dma((1,)), dma((chips, kv_heads)), dma((chips, kv_heads)), dma((chips, kv_heads)),
                dma((2, tp_n - 1, 2)), dma((2, tp_n - 1, 2)), dma((2, tp_n - 1, 2)), dma((2, tp_n - 1, 2)),
            ],
            compiler_params=pltpu.CompilerParams(collective_id=0, has_side_effects=True, vmem_limit_bytes=VMEM_LIMIT),
        )(hidden, positions.reshape(1, rows), norm_gain.reshape(width // HEAD, HEAD), w_query, w_key, w_value, w_out)
        results = (out, k_cache, v_cache)
        return pl.pallas_call(
            store_kernel,
            out_shape=tuple(jax.ShapeDtypeStruct(r.shape, BF16) for r in results),
            in_specs=[vmem_spec] * 3,
            out_specs=(any_spec,) * 3,
            scratch_shapes=[dma((3,))],
        )(*[pltpu.with_memory_space_constraint(r, pltpu.VMEM) for r in results])

    return jax.shard_map(local_block, mesh=mesh, in_specs=(row_spec, P(('dp', 'cp')), P(None), head_cols, head_cols, head_cols, P('tp', None)), out_specs=(row_spec, cache_spec, cache_spec), check_vma=False)
```
